128 devices in a mesh: tok: 64 (over x, y, z), col: 2 (over core).
Axes of the slice: x: 4, y: 4, z: 4, core: 2. Of those that a mesh axis runs over, the one named last changes fastest.
Arguments:
- first_acts: bfloat16 [98304, 4096], P('tok', 'col'), as said below
- second_acts: bfloat16 [98304, 4096], P('tok', 'col'), as said below
- window_counts: int32 [256], P('tok'), may hold values from 96 to 384, as said below
Outputs:
- whitened: float32 [4096, 4096], P('tok', 'col')
- means: float32 [2, 4096], P(None, 'col')
The draws below stay inside these ranges and needn't reach their ends.
Inputs may be any that keep to these rules, and one draw needn't show every extreme that they name: `window_counts`: the live tokens of a window are its first ones; on every index of tok one of its 4 windows is full with 384 live tokens. `first_acts`: real values of order one to some tens; slots that are not live hold values too. `second_acts`: real values of order one to some tens; slots that are not live hold values too.
All inputs are finite; a program needn't handle non-finite values.
Results may differ from the reference program's by a relative error of at most 0.0003.
Values may be sent and summed in bfloat16 or wider, within the bound.
A program may use at most 192 MiB of HBM per device.

```python
import math
import jax
import jax.numpy as jnp
from jax import lax

D = 4096
WINDOWS = 4
SLOTS = 384
TOK_DEV = 1536
TOKENS = 98304
BLOCKS = 256
N_TOK = 64


def paired_draw(key):
    key = jax.random.fold_in(key, 11)
    streams = jax.random.split(key, 8)
    feature_block = D // N_TOK
    base_field = jax.random.normal(streams[0], (TOKENS, D), jnp.float32)
    noise_field = jax.random.normal(streams[1], (TOKENS, D), jnp.float32)
    offset_scale = 1.0
    common_shift = 0.0
    row_scale = jnp.ones((TOKENS,), jnp.float32)
    channel_scale = jnp.exp(jax.random.uniform(streams[2], (D,), jnp.float32, math.log(0.5), math.log(2.0)))
    block_shift = offset_scale * jax.random.normal(streams[3], (BLOCKS, D), jnp.float32) + common_shift
    second_shift = offset_scale * jax.random.normal(streams[6], (BLOCKS, D), jnp.float32)
    pairing = jax.random.permutation(streams[4], N_TOK)
    row_device = jnp.arange(TOKENS, dtype=jnp.int32) // TOK_DEV
    feature_owner = jnp.arange(D, dtype=jnp.int32) // feature_block
    spike_scale = jnp.where(pairing[row_device][:, None] == feature_owner[None, :], 5.0, 1.0)
    first_field = (base_field * channel_scale[None, :] * row_scale[:, None] + jnp.repeat(block_shift, SLOTS, axis=0)) * spike_scale
    second_field = 0.5 * first_field + 0.4 * jnp.roll(first_field, 1, axis=1) + 0.6 * noise_field * channel_scale[None, :] + jnp.repeat(second_shift, SLOTS, axis=0)
    return (first_field, second_field)


def draw_first_acts(key, part):
    return paired_draw(key)[0].astype(jnp.bfloat16)


def draw_second_acts(key, part):
    return paired_draw(key)[1].astype(jnp.bfloat16)


def draw_window_counts(key, part):
    key_counts, key_full = jax.random.split(jax.random.fold_in(key, 29))
    drawn = jax.random.randint(key_counts, (BLOCKS,), SLOTS // 4, SLOTS + 1, jnp.int32)
    chosen = jax.random.randint(key_full, (N_TOK,), 0, WINDOWS, jnp.int32)
    filled = (lax_iota_windows()[None, :] == chosen[:, None]).reshape(BLOCKS)
    return jnp.where(filled, SLOTS, drawn).astype(jnp.int32)


def lax_iota_windows():
    return jnp.arange(WINDOWS, dtype=jnp.int32)


def setup_inputs(seed: int = 0) -> dict:
    key_of = jax.random.split(jax.random.key(seed), 4)
    first_acts = draw_first_acts(jax.random.fold_in(key_of[3], 71), 0)
    second_acts = draw_second_acts(jax.random.fold_in(key_of[3], 71), 0)
    window_counts = draw_window_counts(jax.random.fold_in(key_of[3], 71), 0)
    return {"first_acts": first_acts, "second_acts": second_acts, "window_counts": window_counts}


def reference(first_acts, second_acts, window_counts):
    blocks = window_counts.shape[0]
    first_win = first_acts.reshape(blocks, SLOTS, D)
    second_win = second_acts.reshape(blocks, SLOTS, D)
    live_mask = lax.broadcasted_iota(jnp.int32, (blocks, SLOTS), 1) < window_counts[:, None]
    count_float = window_counts.astype(jnp.float32)
    mean_first = lax.optimization_barrier(jnp.sum(jnp.where(live_mask[:, :, None], first_win.astype(jnp.float32), 0.0), axis=1)) / count_float[:, None]
    mean_second = lax.optimization_barrier(jnp.sum(jnp.where(live_mask[:, :, None], second_win.astype(jnp.float32), 0.0), axis=1)) / count_float[:, None]
    grand_count = jnp.sum(count_float)
    grand_first = lax.optimization_barrier(jnp.sum(count_float[:, None] * mean_first, axis=0)) / grand_count
    grand_second = lax.optimization_barrier(jnp.sum(count_float[:, None] * mean_second, axis=0)) / grand_count

    def accumulate(carry, inputs):
        cross, square_first, square_second = carry
        rows_first, rows_second, live_rows, win_first, win_second = inputs
        centered_first = jnp.where(live_rows[:, None], rows_first - win_first[None, :], 0.0).astype(jnp.bfloat16)
        centered_second = jnp.where(live_rows[:, None], rows_second - win_second[None, :], 0.0).astype(jnp.bfloat16)
        cross = cross + jnp.dot(centered_first.T, centered_second, preferred_element_type=jnp.float32)
        square_first = square_first + lax.optimization_barrier(jnp.sum(jnp.square(centered_first.astype(jnp.float32)), axis=0))
        square_second = square_second + lax.optimization_barrier(jnp.sum(jnp.square(centered_second.astype(jnp.float32)), axis=0))
        return ((cross, square_first, square_second), None)
    start_state = (jnp.zeros((D, D), jnp.float32), jnp.zeros((D,), jnp.float32), jnp.zeros((D,), jnp.float32))
    (cross, square_first, square_second), _ = lax.scan(accumulate, start_state, (first_win, second_win, live_mask, mean_first, mean_second))
    shift_first = mean_first - grand_first[None, :]
    shift_second = mean_second - grand_second[None, :]
    cross = cross + jnp.dot((count_float[:, None] * shift_first).T, shift_second, preferred_element_type=jnp.float32, precision=lax.Precision.HIGHEST)
    var_first = (square_first + lax.optimization_barrier(jnp.sum(count_float[:, None] * jnp.square(shift_first), axis=0))) / grand_count
    var_second = (square_second + lax.optimization_barrier(jnp.sum(count_float[:, None] * jnp.square(shift_second), axis=0))) / grand_count
    whitened = cross / grand_count / jnp.sqrt((var_first[:, None] + 0.1) * (var_second[None, :] + 0.1))
    means = jnp.stack([grand_first, grand_second])
    return (whitened, means)
```

```python
import functools

import jax
import jax.numpy as jnp
from jax import lax
from jax.experimental import pallas as pl
from jax.experimental.pallas import tpu as pltpu
from jax.sharding import Mesh
from jax.sharding import PartitionSpec as P

TOK = ("tok_0", "tok_1", "tok_2")
MESH = pl.DeviceIdType.MESH
STRIDE = (16, 4, 1)
LANE = 128
AUX = 128
CODES = 32767.0
contract_rows = (((0,), (0,)), ((), ()))


def center_kernel(
    counts_ref, first_ref, second_ref, left_ref, right_ref, left_aux, right_aux, stats_ref, means, squares
):
    window = pl.program_id(0)
    windows = pl.num_programs(0)
    slots, width = first_ref.shape
    live_count = counts_ref[window]
    count_float = live_count.astype(jnp.float32)
    live = lax.broadcasted_iota(jnp.int32, (slots, LANE), 0) < live_count
    eight = lax.broadcasted_iota(jnp.int32, (8, LANE), 0)

    @pl.when(window == 0)
    def _():
        squares[...] = jnp.zeros_like(squares)
        means[...] = jnp.zeros_like(means)

    def centered_of(ref, which, cs):
        x = jnp.where(live, ref[:, cs].astype(jnp.float32), 0.0)
        mean = jnp.sum(x, axis=0, keepdims=True) / count_float
        means[which, :, cs] = jnp.where(eight == window, mean, means[which, :, cs])
        centered = jnp.where(live, x - mean, 0.0).astype(jnp.bfloat16)
        wide = centered.astype(jnp.float32)
        squares[which : which + 1, cs] += jnp.sum(wide * wide, axis=0, keepdims=True)
        return centered

    def chunk(j, _):
        cs = pl.ds(pl.multiple_of(j * LANE, LANE), LANE)
        left_ref[cs, :] = centered_of(first_ref, 0, cs).T
        right_ref[:, cs] = centered_of(second_ref, 1, cs)
        return 0

    lax.fori_loop(0, width // LANE, chunk, 0)

    @pl.when(window == windows - 1)
    def _():
        counts = [counts_ref[w].astype(jnp.float32) for w in range(4)]
        total = counts[0] + counts[1] + counts[2] + counts[3]
        row = lax.broadcasted_iota(jnp.int32, (16, LANE), 0)

        def rows_of(which, cs, weighted):
            mean = [means[which, w : w + 1, cs] for w in range(4)]
            device = sum(counts[w] * mean[w] for w in range(4)) / total
            shift = [m - device for m in mean]
            part = squares[which : which + 1, cs] + sum(counts[w] * shift[w] * shift[w] for w in range(4))
            stats_ref[which : which + 1, cs] = device
            stats_ref[which + 2 : which + 3, cs] = part
            packed = jnp.zeros((16, LANE), jnp.float32)
            for w in range(4):
                value = counts[w] * shift[w] if weighted else shift[w]
                high = value.astype(jnp.bfloat16).astype(jnp.float32)
                low = value - high
                order = (high, high, low, low) if weighted else (high, low, high, low)
                for k in range(4):
                    packed = jnp.where(row == 4 * k + w, order[k], packed)
            return jnp.concatenate([packed, jnp.zeros((AUX - 16, LANE), jnp.float32)], axis=0)

        def tail(j, _):
            cs = pl.ds(pl.multiple_of(j * LANE, LANE), LANE)
            left_aux[cs, :] = rows_of(0, cs, True).T.astype(jnp.bfloat16)
            right_aux[:, cs] = rows_of(1, cs, False).astype(jnp.bfloat16)
            return 0

        lax.fori_loop(0, width // LANE, tail, 0)


def center(first_acts, second_acts, window_counts):
    windows = window_counts.shape[0]
    tokens, width = first_acts.shape
    slots = tokens // windows
    bf16 = jnp.bfloat16
    return pl.pallas_call(
        center_kernel,
        grid=(windows,),
        in_specs=[
            pl.BlockSpec(memory_space=pltpu.SMEM),
            pl.BlockSpec((slots, width), lambda w: (w, 0)),
            pl.BlockSpec((slots, width), lambda w: (w, 0)),
        ],
        out_specs=[
            pl.BlockSpec((width, slots), lambda w: (0, w)),
            pl.BlockSpec((slots, width), lambda w: (w, 0)),
            pl.BlockSpec((width, AUX), lambda w: (0, 0)),
            pl.BlockSpec((AUX, width), lambda w: (0, 0)),
            pl.BlockSpec((8, width), lambda w: (0, 0)),
        ],
        out_shape=[
            jax.ShapeDtypeStruct((width, tokens), bf16),
            jax.ShapeDtypeStruct((tokens, width), bf16),
            jax.ShapeDtypeStruct((width, AUX), bf16),
            jax.ShapeDtypeStruct((AUX, width), bf16),
            jax.ShapeDtypeStruct((8, width), jnp.float32),
        ],
        scratch_shapes=[pltpu.VMEM((2, 8, width), jnp.float32), pltpu.VMEM((8, width), jnp.float32)],
        compiler_params=pltpu.CompilerParams(
            dimension_semantics=("arbitrary",), vmem_limit_bytes=48 * 1024 * 1024
        ),
        cost_estimate=pl.CostEstimate(flops=40_000_000, bytes_accessed=28_000_000, transcendentals=0),
        name="center",
    )(window_counts, first_acts, second_acts)


DIMS = ((0, 1, 2), (1, 2, 0), (2, 0, 1))


def widths_of(width):
    tiles = width // LANE
    cut = [tiles // 3 + (1 if q < tiles % 3 else 0) for q in range(3)]
    return [c * LANE for c in cut]


def product_kernel(
    widths,
    left_hbm, right_hbm, left_aux_hbm, right_aux_hbm, out_ref,
    left, right, sums, send1, recv1, sscale1, rscale1, send2, recv2, sscale2, rscale2,
    send3, recv3, sscale3, rscale3,
    local_sem, peer_send, peer_recv, s1, r1, t1, u1, s2, r2, t2, u2, s3, r3, t3, u3,
):
    me = [lax.axis_index(name) for name in TOK]
    core = lax.axis_index("col")
    tokens = left_hbm.shape[2]
    half_blocks = left.shape[0] // 2
    starts = [sum(widths[:q]) for q in range(3)]

    barrier = pltpu.get_barrier_semaphore()
    for d in range(3):
        for step in (1, 3):
            pl.semaphore_signal(
                barrier, inc=1, device_id={TOK[d]: lax.rem(me[d] + step, 4)}, device_id_type=MESH
            )
    pl.semaphore_signal(barrier, inc=1, device_id={"col": 1 - core}, device_id_type=MESH)

    mine = pl.ds(core * half_blocks, half_blocks)
    local = [
        pltpu.make_async_copy(left_hbm, left.at[mine, :, pl.ds(0, tokens)], local_sem.at[0]),
        pltpu.make_async_copy(left_aux_hbm, left.at[mine, :, pl.ds(tokens, AUX)], local_sem.at[1]),
        pltpu.make_async_copy(right_hbm, right.at[pl.ds(0, tokens)], local_sem.at[2]),
        pltpu.make_async_copy(right_aux_hbm, right.at[pl.ds(tokens, AUX)], local_sem.at[3]),
    ]
    for copy in local:
        copy.start()
    pl.semaphore_wait(barrier, 7)
    peer = [
        pltpu.make_async_remote_copy(
            left_hbm, left.at[mine, :, pl.ds(0, tokens)], peer_send.at[0], peer_recv.at[0],
            device_id={"col": 1 - core}, device_id_type=MESH,
        ),
        pltpu.make_async_remote_copy(
            left_aux_hbm, left.at[mine, :, pl.ds(tokens, AUX)], peer_send.at[1], peer_recv.at[1],
            device_id={"col": 1 - core}, device_id_type=MESH,
        ),
    ]
    for copy in peer:
        copy.start()
    for copy in local:
        copy.wait()
    for copy in peer:
        copy.wait()

    def columns(q):
        return pl.ds(starts[q], widths[q])

    def tile(q, j):
        return pl.ds(pl.multiple_of(starts[q] + j * LANE, LANE), LANE)

    def multiply(q, to_a, to_b):
        a, b, g = DIMS[q]
        blocks = []
        for distance in (2, 1, 3, 0):
            to_g = lax.rem(me[g] + distance, 4)
            blocks.append(left[to_a * STRIDE[a] + to_b * STRIDE[b] + to_g * STRIDE[g]])
        sums[:, columns(q)] = jnp.dot(
            jnp.concatenate(blocks, axis=0), right[:, columns(q)], preferred_element_type=jnp.float32
        )

    def encoded(p, code_ref, scale_ref):
        peak = jnp.maximum(jnp.max(jnp.abs(p), axis=0, keepdims=True), 1e-30)
        code = jnp.round(p * (CODES / peak)).astype(jnp.int32)
        code_ref[...] = code.astype(jnp.int16)
        scale_ref[...] = peak * (1.0 / CODES)

    def decoded(code_ref, scale_ref):
        return code_ref[...].astype(jnp.int32).astype(jnp.float32) * scale_ref[...]

    def each_tile(q, body):
        def step(j, _):
            body(tile(q, j))
            return 0

        lax.fori_loop(0, widths[q] // LANE, step, 0)

    def copies1(q, slot, target):
        to = {TOK[DIMS[q][0]]: target}
        cs = columns(q)
        return (
            pltpu.make_async_remote_copy(
                send1.at[slot, :, cs], recv1.at[slot, :, cs], s1.at[q, slot], r1.at[q, slot],
                device_id=to, device_id_type=MESH,
            ),
            pltpu.make_async_remote_copy(
                sscale1.at[slot, :, cs], rscale1.at[slot, :, cs], t1.at[q, slot], u1.at[q, slot],
                device_id=to, device_id_type=MESH,
            ),
        )

    def start(copies):
        for copy in copies:
            copy.start()

    def arrived(copies):
        for copy in copies:
            copy.wait_recv()

    def left_of(copies):
        for copy in copies:
            copy.wait_send()

    def towards(q, i):
        return lax.rem(me[DIMS[q][0]] + 1 + 2 * lax.rem(i, 2), 4)

    def early_far(i, _):
        for q in range(3):
            a, b, g = DIMS[q]
            distance = jnp.where(i < 2, 2 + i, 3 - i)
            multiply(q, lax.rem(me[a] + 2, 4), lax.rem(me[b] + distance, 4))

            def body(cs):
                encoded(sums[:, cs], send1.at[i, :, cs], sscale1.at[i, :, cs])

            each_tile(q, body)
            start(copies1(q, i, towards(q, i)))
        return 0

    def near_plain(i, _):
        for q in range(3):
            a, b, g = DIMS[q]
            distance = jnp.where(i < 2, 3 - i, i - 2)
            multiply(q, towards(q, i), lax.rem(me[b] + distance, 4))

            def body(cs):
                encoded(sums[:, cs], send1.at[4 + i, :, cs], sscale1.at[4 + i, :, cs])

            each_tile(q, body)
            start(copies1(q, 4 + i, towards(q, i)))
        return 0

    def near_adding(i, _):
        for q in range(3):
            a, b, g = DIMS[q]
            distance = jnp.where(i < 2, 2 + i, 3 - i)
            multiply(q, towards(q, i), lax.rem(me[b] + distance, 4))
            arrived(copies1(q, i, towards(q, i)))

            def body(cs):
                p = sums[:, cs] + decoded(recv1.at[i, :, cs], rscale1.at[i, :, cs])
                encoded(p, send1.at[8 + i, :, cs], sscale1.at[8 + i, :, cs])

            each_tile(q, body)
            start(copies1(q, 8 + i, towards(q, i)))
        return 0

    lax.fori_loop(0, 4, early_far, 0)
    lax.fori_loop(0, 4, near_plain, 0)
    lax.fori_loop(0, 4, near_adding, 0)

    rows = sums.shape[0]
    top, bottom = pl.ds(0, rows // 2), pl.ds(rows // 2, rows // 2)

    def copies2(q, slot, part, target):
        to = {TOK[DIMS[q][1]]: target}
        cs = columns(q)
        lines = (top, bottom)[part] if slot == 0 else pl.ds(0, rows)
        k = part if slot == 0 else slot + 1
        return (
            pltpu.make_async_remote_copy(
                send2.at[slot, lines, cs], recv2.at[slot, lines, cs], s2.at[q, k], r2.at[q, k],
                device_id=to, device_id_type=MESH,
            ),
            pltpu.make_async_remote_copy(
                sscale2.at[slot, :, cs], rscale2.at[k, :, cs], t2.at[q, k], u2.at[q, k],
                device_id=to, device_id_type=MESH,
            ),
        )

    def merged1(i, cs):
        low = jnp.where(i < 2, 8 + 2 * i, 2 * i)
        high = 5 + 2 * i
        return (
            sums[:, cs]
            + decoded(recv1.at[low, :, cs], rscale1.at[low, :, cs])
            + decoded(recv1.at[high, :, cs], rscale1.at[high, :, cs])
        )

    def own(i, _):
        for q in range(3):
            a, b, g = DIMS[q]
            after, before = lax.rem(me[b] + 1, 4), lax.rem(me[b] + 3, 4)
            distance = jnp.where(i == 0, 2, jnp.where(i == 1, 1, jnp.where(i == 2, 3, 0)))
            multiply(q, me[a], lax.rem(me[b] + distance, 4))
            arrived(copies1(q, jnp.where(i < 2, 8 + 2 * i, 2 * i), me[a]))
            arrived(copies1(q, 5 + 2 * i, me[a]))

            @pl.when(i == 0)
            def _():
                def body(cs):
                    encoded(merged1(i, cs), send2.at[0, :, cs], sscale2.at[0, :, cs])

                each_tile(q, body)
                start(copies2(q, 0, 0, after))
                start(copies2(q, 0, 1, before))

            @pl.when(i == 1)
            def _():
                arrived(copies2(q, 0, 0, after))

                def body(cs):
                    p = merged1(i, cs)
                    p = jnp.concatenate(
                        [p[: rows // 2] + decoded(recv2.at[0, top, cs], rscale2.at[0, :, cs]), p[rows // 2 :]], axis=0
                    )
                    encoded(p, send2.at[1, :, cs], sscale2.at[1, :, cs])

                each_tile(q, body)
                start(copies2(q, 1, 0, after))

            @pl.when(i == 2)
            def _():
                arrived(copies2(q, 0, 1, before))

                def body(cs):
                    p = merged1(i, cs)
                    p = jnp.concatenate(
                        [p[: rows // 2], p[rows // 2 :] + decoded(recv2.at[0, bottom, cs], rscale2.at[1, :, cs])], axis=0
                    )
                    encoded(p, send2.at[2, :, cs], sscale2.at[2, :, cs])

                each_tile(q, body)
                start(copies2(q, 2, 0, before))

            @pl.when(i == 3)
            def _():
                def body(cs):
                    sums[:, cs] = merged1(i, cs)

                each_tile(q, body)

        return 0

    lax.fori_loop(0, 4, own, 0)

    part_rows = rows // 4
    half = part_rows // 2
    first_half, second_half = pl.ds(0, half), pl.ds(half, half)

    def copies3(q, slot, part, target):
        to = {TOK[DIMS[q][2]]: target}
        cs = columns(q)
        lines = (first_half, second_half)[part] if slot == 0 else pl.ds(0, part_rows)
        k = part if slot == 0 else slot + 1
        return (
            pltpu.make_async_remote_copy(
                send3.at[slot, lines, cs], recv3.at[slot, lines, cs], s3.at[q, k], r3.at[q, k],
                device_id=to, device_id_type=MESH,
            ),
            pltpu.make_async_remote_copy(
                sscale3.at[slot, :, cs], rscale3.at[k, :, cs], t3.at[q, k], u3.at[q, k],
                device_id=to, device_id_type=MESH,
            ),
        )

    def after3(q):
        return lax.rem(me[DIMS[q][2]] + 1, 4)

    def before3(q):
        return lax.rem(me[DIMS[q][2]] + 3, 4)

    for q in range(3):
        arrived(copies2(q, 1, 0, me[DIMS[q][1]]))
        arrived(copies2(q, 2, 0, me[DIMS[q][1]]))

        def body(cs):
            p = (
                sums[:, cs]
                + decoded(recv2.at[1, :, cs], rscale2.at[2, :, cs])
                + decoded(recv2.at[2, :, cs], rscale2.at[3, :, cs])
            )
            encoded(p[:part_rows], send3.at[0, :, cs], sscale3.at[0, :, cs])
            sums[pl.ds(part_rows, 3 * part_rows), cs] = p[part_rows:]

        each_tile(q, body)
        start(copies3(q, 0, 0, after3(q)))
        start(copies3(q, 0, 1, before3(q)))

    for q in range(3):
        arrived(copies3(q, 0, 0, after3(q)))
        arrived(copies3(q, 0, 1, before3(q)))

        def body(cs):
            ahead = jnp.concatenate(
                [
                    sums[pl.ds(part_rows, half), cs] + decoded(recv3.at[0, first_half, cs], rscale3.at[0, :, cs]),
                    sums[pl.ds(part_rows + half, half), cs],
                ],
                axis=0,
            )
            encoded(ahead, send3.at[1, :, cs], sscale3.at[1, :, cs])
            behind = jnp.concatenate(
                [
                    sums[pl.ds(2 * part_rows, half), cs],
                    sums[pl.ds(2 * part_rows + half, half), cs]
                    + decoded(recv3.at[0, second_half, cs], rscale3.at[1, :, cs]),
                ],
                axis=0,
            )
            encoded(behind, send3.at[2, :, cs], sscale3.at[2, :, cs])

        each_tile(q, body)
        start(copies3(q, 1, 0, after3(q)))
        start(copies3(q, 2, 0, before3(q)))

    for q in range(3):
        arrived(copies3(q, 1, 0, after3(q)))
        arrived(copies3(q, 2, 0, before3(q)))

        def body(cs):
            out_ref[:, cs] = (
                sums[pl.ds(3 * part_rows, part_rows), cs]
                + decoded(recv3.at[1, :, cs], rscale3.at[2, :, cs])
                + decoded(recv3.at[2, :, cs], rscale3.at[3, :, cs])
            )

        each_tile(q, body)

    def drain(i, _):
        for q in range(3):
            left_of(copies1(q, i, towards(q, i)))
        return 0

    lax.fori_loop(0, 12, drain, 0)
    for q in range(3):
        for copies, towards_next, towards_last in (
            (copies2, lax.rem(me[DIMS[q][1]] + 1, 4), lax.rem(me[DIMS[q][1]] + 3, 4)),
            (copies3, after3(q), before3(q)),
        ):
            left_of(copies(q, 0, 0, towards_next))
            left_of(copies(q, 0, 1, towards_last))
            left_of(copies(q, 1, 0, towards_next))
            left_of(copies(q, 2, 0, towards_last))


def product(left, right, left_aux, right_aux):
    half_width, tokens = left.shape
    width = right.shape[1]
    block = 2 * half_width // 64
    blocks = half_width // block
    left = left.reshape(blocks, block, tokens)
    left_aux = left_aux.reshape(blocks, block, AUX)
    rows = 4 * block
    depth = tokens + AUX
    i16, f32 = jnp.int16, jnp.float32
    dma = pltpu.SemaphoreType.DMA
    return pl.pallas_call(
        functools.partial(product_kernel, widths_of(width)),
        out_shape=jax.ShapeDtypeStruct((block, width), f32),
        in_specs=[pl.BlockSpec(memory_space=pl.ANY)] * 4,
        out_specs=pl.BlockSpec(memory_space=pltpu.VMEM),
        scratch_shapes=[
            pltpu.VMEM((2 * blocks, block, depth), jnp.bfloat16),
            pltpu.VMEM((depth, width), jnp.bfloat16),
            pltpu.VMEM((rows, width), f32),
            pltpu.VMEM((12, rows, width), i16),
            pltpu.VMEM((12, rows, width), i16),
            pltpu.VMEM((12, 1, width), f32),
            pltpu.VMEM((12, 1, width), f32),
            pltpu.VMEM((3, rows, width), i16),
            pltpu.VMEM((3, rows, width), i16),
            pltpu.VMEM((3, 1, width), f32),
            pltpu.VMEM((4, 1, width), f32),
            pltpu.VMEM((3, block, width), i16),
            pltpu.VMEM((3, block, width), i16),
            pltpu.VMEM((3, 1, width), f32),
            pltpu.VMEM((4, 1, width), f32),
            dma((4,)), dma((2,)), dma((2,)),
            dma((3, 12)), dma((3, 12)), dma((3, 12)), dma((3, 12)),
            dma((3, 4)), dma((3, 4)), dma((3, 4)), dma((3, 4)),
            dma((3, 4)), dma((3, 4)), dma((3, 4)), dma((3, 4)),
        ],
        compiler_params=pltpu.CompilerParams(
            collective_id=0, has_side_effects=True, vmem_limit_bytes=67_000_000
        ),
        cost_estimate=pl.CostEstimate(
            flops=4 * half_width * width * depth, bytes_accessed=30_000_000, transcendentals=0
        ),
        name="product",
    )(left, right, left_aux, right_aux)


def local(first_acts, second_acts, window_counts):
    half_width = first_acts.shape[1]
    col_index = lax.axis_index("col")
    full_width = half_width * lax.axis_size("col")
    row_width = full_width // lax.axis_size(TOK)
    row_offset = lax.axis_index(TOK) * row_width
    left, right, left_aux, right_aux, stats = center(first_acts, second_acts, window_counts)
    device_count = jnp.sum(window_counts.astype(jnp.float32))
    first_stats = lax.all_gather(stats[0:3:2], "col", axis=1, tiled=True)
    row = jnp.concatenate(
        [first_stats[0], stats[1], first_stats[1], stats[3], device_count.reshape(1)]
    )
    peers = lax.all_gather(row[None], TOK, axis=0, tiled=True)
    cross = product(left, right, left_aux, right_aux)
    peer_count = peers[:, -1]
    f, h = full_width, half_width
    grand_count = jnp.sum(peer_count)
    peer_mean = peers[:, : f + h]
    peer_part = peers[:, f + h : 2 * (f + h)]
    grand = jnp.sum(peer_count[:, None] * peer_mean, axis=0) / grand_count
    shift = peer_mean - grand[None, :]
    var = (jnp.sum(peer_part, axis=0) + jnp.sum(peer_count[:, None] * jnp.square(shift), axis=0)) / grand_count
    late_left = lax.dynamic_slice_in_dim(shift, row_offset, row_width, 1) * peer_count[:, None]
    cross = cross + lax.dot_general(
        late_left,
        shift[:, f:],
        contract_rows,
        precision=lax.Precision.HIGHEST,
        preferred_element_type=jnp.float32,
    )
    var_first = lax.dynamic_slice_in_dim(var, row_offset, row_width)
    var_second = var[f:]
    whitened = cross / grand_count / jnp.sqrt((var_first[:, None] + 0.1) * (var_second[None, :] + 0.1))
    means = jnp.stack([lax.dynamic_slice_in_dim(grand, col_index * half_width, half_width), grand[f:]])
    return (whitened, means)


def solution(mesh):
    torus = Mesh(
        mesh.devices.reshape(4, 4, 4, mesh.shape["col"]), ("tok_0", "tok_1", "tok_2", "col")
    )
    return jax.shard_map(
        local,
        mesh=torus,
        in_specs=(P(TOK, "col"), P(TOK, "col"), P(TOK)),
        out_specs=(P(TOK, "col"), P(None, "col")),
        check_vma=False,
    )
```

```python
import functools

import jax
import jax.numpy as jnp
from jax import lax
from jax.experimental import pallas as pl
from jax.experimental.pallas import tpu as pltpu
from jax.sharding import Mesh
from jax.sharding import PartitionSpec as P

TOK = ("tok_0", "tok_1", "tok_2")
MESH = pl.DeviceIdType.MESH
LANE = 128
AUX = 128
CODES = 32767.0

DISTANCES = (2, 1, 3, 0)


def widths_of(width):
    tiles = width // LANE
    return [(tiles // 3 + (1 if q < tiles % 3 else 0)) * LANE for q in range(3)]


def pick(k, values):
    result = values[-1]
    for n in range(len(values) - 2, -1, -1):
        result = jnp.where(k == n, values[n], result)
    return result


def kernel(
    widths,
    counts_ref, first_hbm, second_hbm, out_ref, means_ref,
    raw, left, right, sums, far_out, far_in, near_out, near_in, last_out, last_in, mid_in,
    far_scale, far_scale_in, near_scale, near_scale_in, mid_scale, mid_scale_in, last_scale, last_scale_in,
    means, squares, stats, spread_first, column,
    load_sem, peer_send, peer_recv, stat_send, stat_recv, spread_send, spread_recv,
    far_s, far_r, far_t, far_u, near_s, near_r, near_t, near_u,
    mid_s, mid_r, mid_t, mid_u, last_s, last_r, last_t, last_u,
):
    me = [lax.axis_index(name) for name in TOK]
    core = lax.axis_index("col")
    tokens, width = raw.shape
    slots = tokens // 4
    half_blocks = left.shape[0] // 2
    block = left.shape[1]
    starts = [sum(widths[:q]) for q in range(3)]
    rows = sums.shape[0]
    upper, lower = pl.ds(0, rows // 2), pl.ds(rows // 2, rows // 2)

    def at(axis, coordinate):
        return {TOK[d]: jnp.where(axis == d, coordinate, me[d]) for d in range(3)}

    other = {"col": 1 - core}

    loads = []
    for w in range(4):
        lines = pl.ds(w * slots, slots)
        loads.append(pltpu.make_async_copy(first_hbm.at[lines], raw.at[lines], load_sem.at[0, w]))
    for w in range(4):
        lines = pl.ds(w * slots, slots)
        loads.append(pltpu.make_async_copy(second_hbm.at[lines], right.at[lines], load_sem.at[1, w]))
    for copy in loads:
        copy.start()
    barrier = pltpu.get_barrier_semaphore()
    for d in range(3):
        for step in (1, 2, 3):
            pl.semaphore_signal(
                barrier, inc=1, device_id={TOK[d]: lax.rem(me[d] + step, 4)}, device_id_type=MESH
            )
    pl.semaphore_signal(barrier, inc=1, device_id=other, device_id_type=MESH)

    count = [counts_ref[w].astype(jnp.float32) for w in range(4)]
    device_count = count[0] + count[1] + count[2] + count[3]
    row = lax.broadcasted_iota(jnp.int32, (8, tokens), 0)
    slot = lax.broadcasted_iota(jnp.int32, (8, tokens), 1)
    live_rows = jnp.zeros((8, tokens), jnp.float32)
    for w in range(4):
        inside = (row == w) & (slot >= w * slots) & (slot < w * slots + counts_ref[w])
        live_rows = jnp.where(inside, 1.0, live_rows)
    live_rows = live_rows.astype(jnp.bfloat16)
    eight = lax.broadcasted_iota(jnp.int32, (8, LANE), 0)
    count_rows = jnp.ones((8, LANE), jnp.float32)
    weight_rows = jnp.zeros((8, LANE), jnp.float32)
    for w in range(4):
        count_rows = jnp.where(eight == w, count[w], count_rows)
        weight_rows = jnp.where(eight == w, count[w], weight_rows)

    def cs_of(j):
        return pl.ds(pl.multiple_of(j * LANE, LANE), LANE)

    def loop(n, body):
        def step(j, _):
            body(j)
            return 0

        lax.fori_loop(0, n, step, 0)

    squares[...] = jnp.zeros_like(squares)
    for which, ref in ((0, raw), (1, right)):
        for w in range(4):
            loads[4 * which + w].wait()
        means[which] = jnp.dot(live_rows, ref[pl.ds(0, tokens), :], preferred_element_type=jnp.float32)

    pl.semaphore_wait(barrier, 10)

    def stat_copies(kind, d):
        send, recv = ((stat_send, stat_recv), (spread_send, spread_recv))[kind]
        copies = []
        for step in (1, 2, 3):
            to = lax.rem(me[d] + step, 4)
            copies.append(
                pltpu.make_async_remote_copy(
                    stats.at[kind, d, me[d]], stats.at[kind, d, me[d]], send.at[d, step - 1], recv.at[d, me[d]],
                    device_id={TOK[d]: to}, device_id_type=MESH,
                )
            )
        return copies

    def stat_arrivals(kind, d):
        recv = (stat_recv, spread_recv)[kind]
        send = (stat_send, spread_send)[kind]
        for step in (1, 2, 3):
            source = lax.rem(me[d] + step, 4)
            pltpu.make_async_remote_copy(
                stats.at[kind, d, source], stats.at[kind, d, source], send.at[d, step - 1], recv.at[d, source],
                device_id={TOK[d]: source}, device_id_type=MESH,
            ).wait_recv()

    def stat_sum(kind, d):
        return stats[kind, d, 0] + stats[kind, d, 1] + stats[kind, d, 2] + stats[kind, d, 3]

    def stat_start(kind, d):
        for copy in stat_copies(kind, d):
            copy.start()

    def stat_next(kind, d):
        stat_arrivals(kind, d)
        stats[kind, d + 1, me[d + 1]] = stat_sum(kind, d)
        stat_start(kind, d + 1)

    for which in (0, 1):
        stats[0, 0, me[0], which] = jnp.sum(means[which], axis=0, keepdims=True)
    stats[0, 0, me[0], 2] = jnp.full((1, width), device_count, jnp.float32)
    stat_start(0, 0)

    def to_means(j):
        cs = cs_of(j)
        for which in (0, 1):
            means[which, :, cs] = means[which, :, cs] / count_rows

    loop(width // LANE, to_means)

    mine = pl.ds(core * half_blocks, half_blocks)
    groups = LANE // block

    def push(k, lanes):
        return pltpu.make_async_remote_copy(
            left.at[mine, :, lanes], left.at[mine, :, lanes], peer_send.at[k], peer_recv.at[k],
            device_id=other, device_id_type=MESH,
        )

    def window_push(w):
        return push(w, pl.ds(w * slots, slots))

    def aux_push():
        return push(4, pl.ds(tokens, AUX))

    def center(w):
        live = lax.broadcasted_iota(jnp.int32, (slots, LANE), 0) < counts_ref[w]
        lines = pl.ds(w * slots, slots)

        def centered_of(ref, which, cs):
            mean = means[which, w : w + 1, cs]
            x = jnp.where(live, ref[lines, cs].astype(jnp.float32) - mean, 0.0).astype(jnp.bfloat16)
            wide = x.astype(jnp.float32)
            squares[which, :, cs] += jnp.sum((wide * wide).reshape(slots // 8, 8, LANE), axis=0)
            return x

        def chunk(j):
            cs = cs_of(j)
            turned = centered_of(raw, 0, cs).T
            for k in range(groups):
                left[core * half_blocks + j * groups + k, :, lines] = turned[k * block : (k + 1) * block]
            right[lines, cs] = centered_of(right, 1, cs)

        loop(width // LANE, chunk)
        window_push(w).start()

    center(0)
    stat_next(0, 0)
    center(1)
    stat_next(0, 1)
    center(2)
    stat_arrivals(0, 2)
    total = stat_sum(0, 2)
    grand_count = total[2, 0, 0]
    for which in (0, 1):
        means_ref[which : which + 1, :] = total[which] / total[2]

    row16 = lax.broadcasted_iota(jnp.int32, (16, LANE), 0)

    def aux_rows(which, cs, weighted):
        grand = means_ref[which : which + 1, cs]
        packed = jnp.zeros((16, LANE), jnp.float32)
        for w in range(4):
            value = means[which, w : w + 1, cs] - grand
            if weighted:
                value = count[w] * value
            high = value.astype(jnp.bfloat16).astype(jnp.float32)
            low = value - high
            order = (high, high, low, low) if weighted else (high, low, high, low)
            for k in range(4):
                packed = jnp.where(row16 == 4 * k + w, order[k], packed)
        return jnp.concatenate([packed, jnp.zeros((AUX - 16, LANE), jnp.float32)], axis=0)

    def aux(j):
        cs = cs_of(j)
        turned = aux_rows(0, cs, True).T.astype(jnp.bfloat16)
        for k in range(groups):
            left[core * half_blocks + j * groups + k, :, pl.ds(tokens, AUX)] = turned[k * block : (k + 1) * block]
        right[pl.ds(tokens, AUX), cs] = aux_rows(1, cs, False).astype(jnp.bfloat16)

    loop(width // LANE, aux)
    aux_push().start()
    center(3)

    def spread(j):
        cs = cs_of(j)
        for which in (0, 1):
            shift = means[which, :, cs] - means_ref[which : which + 1, cs]
            part = squares[which, :, cs] + weight_rows * shift * shift
            stats[1, 0, me[0], which, :, cs] = jnp.sum(part, axis=0, keepdims=True)

    stats[1, 0, me[0], 2] = jnp.zeros((1, width), jnp.float32)
    loop(width // LANE, spread)
    stat_start(1, 0)

    pushes = [window_push(w) for w in range(4)] + [aux_push()]
    for copy in pushes:
        copy.wait_recv()

    axes = [[lax.rem(core + q + k, 3) for k in range(3)] for q in range(3)]
    here = [[pick(axes[q][k], me) for k in range(3)] for q in range(3)]
    stride = [[pick(axes[q][k], (16, 4, 1)) for k in range(3)] for q in range(3)]

    def columns(q):
        return pl.ds(starts[q], widths[q])

    def moved(q, k, step):
        return lax.rem(here[q][k] + step, 4)

    def device(q, k, step):
        return at(axes[q][k], moved(q, k, step))

    def distance_of(k):
        return pick(k, DISTANCES)

    def multiply(q, first_step, second_step):
        base = moved(q, 0, first_step) * stride[q][0] + moved(q, 1, second_step) * stride[q][1]
        blocks = [left[base + moved(q, 2, distance) * stride[q][2]] for distance in DISTANCES]
        sums[:, columns(q)] = jnp.dot(
            jnp.concatenate(blocks, axis=0), right[:, columns(q)], preferred_element_type=jnp.float32
        )

    def encoded(p, code_ref, scale_ref):
        peak = jnp.maximum(jnp.max(jnp.abs(p), axis=0, keepdims=True), 1e-30)
        code = jnp.round(p * (CODES / peak)).astype(jnp.int32)
        code_ref[...] = code.astype(jnp.int16)
        scale_ref[...] = peak * (1.0 / CODES)

    def decoded(code_ref, scale_ref):
        return code_ref[...].astype(jnp.int32).astype(jnp.float32) * scale_ref[...]

    def each_tile(q, body):
        def step(j):
            body(pl.ds(pl.multiple_of(starts[q] + j * LANE, LANE), LANE))

        loop(widths[q] // LANE, step)

    def pair(code, code_to, scale, scale_to, sems, index, to):
        s, r, t, u = sems
        return (
            pltpu.make_async_remote_copy(
                code, code_to, s.at[index], r.at[index], device_id=to, device_id_type=MESH
            ),
            pltpu.make_async_remote_copy(
                scale, scale_to, t.at[index], u.at[index], device_id=to, device_id_type=MESH
            ),
        )

    far_sems = (far_s, far_r, far_t, far_u)
    near_sems = (near_s, near_r, near_t, near_u)
    mid_sems = (mid_s, mid_r, mid_t, mid_u)
    last_sems = (last_s, last_r, last_t, last_u)

    def far(q, k, way):
        cs = columns(q)
        lines = (upper, lower)[way]
        return pair(
            far_out.at[k, lines, cs], far_in.at[k, lines, cs],
            far_scale.at[k, :, cs], far_scale_in.at[2 * k + way, :, cs],
            far_sems, (q, 2 * k + way), device(q, 0, (1, 3)[way]),
        )

    def near(q, n, step):
        cs = columns(q)
        return pair(
            near_out.at[n, :, cs], near_in.at[n, :, cs], near_scale.at[n, :, cs], near_scale_in.at[n, :, cs],
            near_sems, (q, n), device(q, 0, step),
        )

    def start(copies):
        for copy in copies:
            copy.start()

    def arrived(copies):
        for copy in copies:
            copy.wait_recv()

    def gone(copies):
        for copy in copies:
            copy.wait_send()

    def serve_far(k):
        for q in range(3):
            multiply(q, 2, distance_of(k))

            def body(cs):
                encoded(sums[:, cs], far_out.at[k, :, cs], far_scale.at[k, :, cs])

            each_tile(q, body)
            start(far(q, k, 0))
            start(far(q, k, 1))

    def serve_near(k):
        for way in (0, 1):
            for q in range(3):
                step = (1, 3)[way]
                multiply(q, step, distance_of(k))
                arrived(far(q, k, way))
                n = 2 * k + way

                def body(cs):
                    p = sums[:, cs]
                    more = decoded(far_in.at[k, (upper, lower)[way], cs], far_scale_in.at[n, :, cs])
                    if way == 0:
                        p = jnp.concatenate([p[: rows // 2] + more, p[rows // 2 :]], axis=0)
                    else:
                        p = jnp.concatenate([p[: rows // 2], p[rows // 2 :] + more], axis=0)
                    encoded(p, near_out.at[n, :, cs], near_scale.at[n, :, cs])

                each_tile(q, body)
                start(near(q, n, step))

    loop(4, serve_far)
    stat_next(1, 0)
    loop(2, serve_near)
    stat_next(1, 1)
    loop(2, lambda k: serve_near(k + 2))
    stat_arrivals(1, 2)
    spread_first[core] = stat_sum(1, 2)
    spread_push = pltpu.make_async_remote_copy(
        spread_first.at[core], spread_first.at[core], peer_send.at[5], peer_recv.at[5],
        device_id=other, device_id_type=MESH,
    )
    spread_push.start()

    def far_gone(k):
        for q in range(3):
            gone(far(q, k, 0))
            gone(far(q, k, 1))

    loop(4, far_gone)
    mid_out = far_out

    def mid(q, n, way=0):
        cs = columns(q)
        lines = (upper, lower)[way] if n == 0 else pl.ds(0, rows)
        k = way if n == 0 else n + 1
        step = (1, 3)[way] if n == 0 else (1, 3)[n - 1]
        return pair(
            mid_out.at[n, lines, cs], mid_in.at[n, lines, cs], mid_scale.at[n, :, cs], mid_scale_in.at[k, :, cs],
            mid_sems, (q, k), device(q, 1, step),
        )

    def merged(k, cs):
        n = 2 * k
        return (
            sums[:, cs]
            + decoded(near_in.at[n, :, cs], near_scale_in.at[n, :, cs])
            + decoded(near_in.at[n + 1, :, cs], near_scale_in.at[n + 1, :, cs])
        )

    def own(k):
        for q in range(3):
            multiply(q, 0, distance_of(k))
            arrived(near(q, 2 * k, 1))
            arrived(near(q, 2 * k + 1, 3))

            @pl.when(k == 0)
            def _():
                def body(cs):
                    encoded(merged(k, cs), mid_out.at[0, :, cs], mid_scale.at[0, :, cs])

                each_tile(q, body)
                start(mid(q, 0, 0))
                start(mid(q, 0, 1))

            @pl.when(k == 1)
            def _():
                arrived(mid(q, 0, 0))

                def body(cs):
                    p = merged(k, cs)
                    more = decoded(mid_in.at[0, upper, cs], mid_scale_in.at[0, :, cs])
                    p = jnp.concatenate([p[: rows // 2] + more, p[rows // 2 :]], axis=0)
                    encoded(p, mid_out.at[1, :, cs], mid_scale.at[1, :, cs])

                each_tile(q, body)
                start(mid(q, 1))

            @pl.when(k == 2)
            def _():
                arrived(mid(q, 0, 1))

                def body(cs):
                    p = merged(k, cs)
                    more = decoded(mid_in.at[0, lower, cs], mid_scale_in.at[1, :, cs])
                    p = jnp.concatenate([p[: rows // 2], p[rows // 2 :] + more], axis=0)
                    encoded(p, mid_out.at[2, :, cs], mid_scale.at[2, :, cs])

                each_tile(q, body)
                start(mid(q, 2))

            @pl.when(k == 3)
            def _():
                def body(cs):
                    sums[:, cs] = merged(k, cs)

                each_tile(q, body)

    loop(4, own)

    part = rows // 4
    half = part // 2
    front, back = pl.ds(0, half), pl.ds(half, half)

    def last(q, n, way=0):
        cs = columns(q)
        lines = (front, back)[way] if n == 0 else pl.ds(0, part)
        k = way if n == 0 else n + 1
        step = (1, 3)[way] if n == 0 else (1, 3)[n - 1]
        return pair(
            last_out.at[n, lines, cs], last_in.at[n, lines, cs], last_scale.at[n, :, cs], last_scale_in.at[k, :, cs],
            last_sems, (q, k), device(q, 2, step),
        )

    for q in range(3):
        arrived(mid(q, 1))
        arrived(mid(q, 2))

        def body(cs):
            p = (
                sums[:, cs]
                + decoded(mid_in.at[1, :, cs], mid_scale_in.at[2, :, cs])
                + decoded(mid_in.at[2, :, cs], mid_scale_in.at[3, :, cs])
            )
            encoded(p[:part], last_out.at[0, :, cs], last_scale.at[0, :, cs])
            sums[pl.ds(part, 3 * part), cs] = p[part:]

        each_tile(q, body)
        start(last(q, 0, 0))
        start(last(q, 0, 1))

    for q in range(3):
        arrived(last(q, 0, 0))
        arrived(last(q, 0, 1))

        def body(cs):
            ahead = jnp.concatenate(
                [
                    sums[pl.ds(part, half), cs] + decoded(last_in.at[0, front, cs], last_scale_in.at[0, :, cs]),
                    sums[pl.ds(part + half, half), cs],
                ],
                axis=0,
            )
            encoded(ahead, last_out.at[1, :, cs], last_scale.at[1, :, cs])
            behind = jnp.concatenate(
                [
                    sums[pl.ds(2 * part, half), cs],
                    sums[pl.ds(2 * part + half, half), cs]
                    + decoded(last_in.at[0, back, cs], last_scale_in.at[1, :, cs]),
                ],
                axis=0,
            )
            encoded(behind, last_out.at[2, :, cs], last_scale.at[2, :, cs])

        each_tile(q, body)
        start(last(q, 1))
        start(last(q, 2))

    spread_push.wait_recv()
    row_block = me[0] * 16 + me[1] * 4 + me[2]
    in_half = lax.rem(row_block, half_blocks)
    lane_block = cs_of(in_half * block // LANE)
    line = spread_first[row_block // half_blocks, 0, :, lane_block] / grand_count
    column[...] = jnp.broadcast_to(line, (LANE, LANE)).T
    rows_var = column[pl.ds(pl.multiple_of(lax.rem(in_half, groups) * block, block), block), :] + 0.1

    for q in range(3):
        arrived(last(q, 1))
        arrived(last(q, 2))

        def body(cs):
            cross = (
                sums[pl.ds(3 * part, part), cs]
                + decoded(last_in.at[1, :, cs], last_scale_in.at[2, :, cs])
                + decoded(last_in.at[2, :, cs], last_scale_in.at[3, :, cs])
            )
            columns_var = spread_first[core, 1, :, cs] / grand_count + 0.1
            out_ref[:, cs] = cross / grand_count * lax.rsqrt(rows_var * columns_var)

        each_tile(q, body)

    def near_gone(k):
        for q in range(3):
            gone(near(q, 2 * k, 1))
            gone(near(q, 2 * k + 1, 3))

    loop(4, near_gone)
    for q in range(3):
        for copies in (mid, last):
            gone(copies(q, 0, 0))
            gone(copies(q, 0, 1))
            gone(copies(q, 1))
            gone(copies(q, 2))
    for copy in pushes + [spread_push]:
        copy.wait_send()
    for kind in (0, 1):
        for d in range(3):
            for copy in stat_copies(kind, d):
                copy.wait_send()


def local(first_acts, second_acts, window_counts):
    tokens, width = first_acts.shape
    block = width * lax.axis_size("col") // lax.axis_size(TOK)
    blocks = width // block
    rows, depth = 4 * block, tokens + AUX
    i16, f32, bf16 = jnp.int16, jnp.float32, jnp.bfloat16
    dma = pltpu.SemaphoreType.DMA
    vmem = pltpu.VMEM
    return pl.pallas_call(
        functools.partial(kernel, widths_of(width)),
        out_shape=(jax.ShapeDtypeStruct((block, width), f32), jax.ShapeDtypeStruct((2, width), f32)),
        in_specs=[
            pl.BlockSpec(memory_space=pltpu.SMEM),
            pl.BlockSpec(memory_space=pl.ANY),
            pl.BlockSpec(memory_space=pl.ANY),
        ],
        out_specs=(pl.BlockSpec(memory_space=vmem), pl.BlockSpec(memory_space=vmem)),
        scratch_shapes=[
            vmem((tokens, width), bf16),
            vmem((2 * blocks, block, depth), bf16),
            vmem((depth, width), bf16),
            vmem((rows, width), f32),
            vmem((4, rows, width), i16), vmem((4, rows, width), i16),
            vmem((8, rows, width), i16), vmem((8, rows, width), i16),
            vmem((3, block, width), i16), vmem((3, block, width), i16),
            vmem((3, rows, width), i16),
            vmem((4, 1, width), f32), vmem((8, 1, width), f32),
            vmem((8, 1, width), f32), vmem((8, 1, width), f32),
            vmem((3, 1, width), f32), vmem((4, 1, width), f32),
            vmem((3, 1, width), f32), vmem((4, 1, width), f32),
            vmem((2, 8, width), f32), vmem((2, 8, width), f32),
            vmem((2, 3, 4, 3, 1, width), f32),
            vmem((2, 3, 1, width), f32),
            vmem((LANE, LANE), f32),
            dma((2, 4)), dma((6,)), dma((6,)),
            dma((3, 3)), dma((3, 4)), dma((3, 3)), dma((3, 4)),
            dma((3, 8)), dma((3, 8)), dma((3, 8)), dma((3, 8)),
            dma((3, 8)), dma((3, 8)), dma((3, 8)), dma((3, 8)),
            dma((3, 4)), dma((3, 4)), dma((3, 4)), dma((3, 4)),
            dma((3, 4)), dma((3, 4)), dma((3, 4)), dma((3, 4)),
        ],
        compiler_params=pltpu.CompilerParams(
            collective_id=0, has_side_effects=True, vmem_limit_bytes=67_043_328
        ),
        cost_estimate=pl.CostEstimate(
            flops=4 * width * width * depth, bytes_accessed=30_000_000, transcendentals=0
        ),
        name="whole",
    )(window_counts, first_acts, second_acts)


def solution(mesh):
    torus = Mesh(
        mesh.devices.reshape(4, 4, 4, mesh.shape["col"]), ("tok_0", "tok_1", "tok_2", "col")
    )
    return jax.shard_map(
        local,
        mesh=torus,
        in_specs=(P(TOK, "col"), P(TOK, "col"), P(TOK)),
        out_specs=(P(TOK, "col"), P(None, "col")),
        check_vma=False,
    )
```

```python
import functools

import jax
import jax.numpy as jnp
from jax import lax
from jax.experimental import pallas as pl
from jax.experimental.pallas import tpu as pltpu
from jax.sharding import Mesh
from jax.sharding import PartitionSpec as P

TOK = ("tok_0", "tok_1", "tok_2")
MESH = pl.DeviceIdType.MESH
LANE = 128
AUX = 128
CODES = 32767.0

DISTANCES = (2, 1, 3, 0)


def widths_of(width):
    tiles = width // LANE
    return [(tiles // 3 + (1 if q < tiles % 3 else 0)) * LANE for q in range(3)]


def pick(k, values):
    result = values[-1]
    for n in range(len(values) - 2, -1, -1):
        result = jnp.where(k == n, values[n], result)
    return result


def kernel(
    widths,
    counts_ref, first_hbm, second_hbm, out_ref, means_ref,
    left, right, far_out, far_in, near_out, near_in, last_out, last_in, mid_in,
    far_scale, far_scale_in, near_scale, near_scale_in, mid_scale, mid_scale_in, last_scale, last_scale_in,
    means, squares, stats, spread_first, column,
    load_sem, peer_send, peer_recv, stat_send, stat_recv, spread_send, spread_recv,
    far_s, far_r, far_t, far_u, near_s, near_r, near_t, near_u,
    mid_s, mid_r, mid_t, mid_u, last_s, last_r, last_t, last_u,
):
    me = [lax.axis_index(name) for name in TOK]
    core = lax.axis_index("col")
    width = right.shape[1]
    tokens = right.shape[0] - AUX
    slots = tokens // 4
    half_blocks = left.shape[0] // 2
    block = left.shape[1]
    starts = [sum(widths[:q]) for q in range(3)]
    rows = far_out.shape[1]
    upper, lower = pl.ds(0, rows // 2), pl.ds(rows // 2, rows // 2)

    def at(axis, coordinate):
        return {TOK[d]: jnp.where(axis == d, coordinate, me[d]) for d in range(3)}

    other = {"col": 1 - core}

    def cs_of(j):
        return pl.ds(pl.multiple_of(j * LANE, LANE), LANE)

    def loop(n, body):
        def step(j, _):
            body(j)
            return 0

        lax.fori_loop(0, n, step, 0)

    def stat_copies(kind, d):
        send, recv = ((stat_send, stat_recv), (spread_send, spread_recv))[kind]
        copies = []
        for step in (1, 2, 3):
            to = lax.rem(me[d] + step, 4)
            copies.append(
                pltpu.make_async_remote_copy(
                    stats.at[kind, d, me[d]], stats.at[kind, d, me[d]], send.at[d, step - 1], recv.at[d, me[d]],
                    device_id={TOK[d]: to}, device_id_type=MESH,
                )
            )
        return copies

    def stat_arrivals(kind, d):
        recv = (stat_recv, spread_recv)[kind]
        send = (stat_send, spread_send)[kind]
        for step in (1, 2, 3):
            source = lax.rem(me[d] + step, 4)
            pltpu.make_async_remote_copy(
                stats.at[kind, d, source], stats.at[kind, d, source], send.at[d, step - 1], recv.at[d, source],
                device_id={TOK[d]: source}, device_id_type=MESH,
            ).wait_recv()

    def stat_sum(kind, d):
        return stats[kind, d, 0] + stats[kind, d, 1] + stats[kind, d, 2] + stats[kind, d, 3]

    def stat_start(kind, d):
        for copy in stat_copies(kind, d):
            copy.start()

    def stat_next(kind, d):
        stat_arrivals(kind, d)
        stats[kind, d + 1, me[d + 1]] = stat_sum(kind, d)
        stat_start(kind, d + 1)

    mine = pl.ds(core * half_blocks, half_blocks)
    groups = LANE // block

    def push(k, lanes):
        return pltpu.make_async_remote_copy(
            left.at[mine, :, lanes], left.at[mine, :, lanes], peer_send.at[k], peer_recv.at[k],
            device_id=other, device_id_type=MESH,
        )

    def window_push(w):
        return push(w, pl.ds(w * slots, slots))

    def aux_push():
        return push(4, pl.ds(tokens, AUX))

    pushes = [window_push(w) for w in range(4)] + [aux_push()]

    def prepare(raw):
        loads = []
        for w in range(4):
            lines = pl.ds(w * slots, slots)
            loads.append(pltpu.make_async_copy(first_hbm.at[lines], raw.at[lines], load_sem.at[0, w]))
        for w in range(4):
            lines = pl.ds(w * slots, slots)
            loads.append(pltpu.make_async_copy(second_hbm.at[lines], right.at[lines], load_sem.at[1, w]))
        for copy in loads:
            copy.start()
        barrier = pltpu.get_barrier_semaphore()
        for d in range(3):
            for step in (1, 2, 3):
                pl.semaphore_signal(
                    barrier, inc=1, device_id={TOK[d]: lax.rem(me[d] + step, 4)}, device_id_type=MESH
                )
        pl.semaphore_signal(barrier, inc=1, device_id=other, device_id_type=MESH)

        count = [counts_ref[w].astype(jnp.float32) for w in range(4)]
        device_count = count[0] + count[1] + count[2] + count[3]
        row = lax.broadcasted_iota(jnp.int32, (8, tokens), 0)
        slot = lax.broadcasted_iota(jnp.int32, (8, tokens), 1)
        live_rows = jnp.zeros((8, tokens), jnp.float32)
        for w in range(4):
            inside = (row == w) & (slot >= w * slots) & (slot < w * slots + counts_ref[w])
            live_rows = jnp.where(inside, 1.0, live_rows)
        live_rows = live_rows.astype(jnp.bfloat16)
        eight = lax.broadcasted_iota(jnp.int32, (8, LANE), 0)
        count_rows = jnp.ones((8, LANE), jnp.float32)
        weight_rows = jnp.zeros((8, LANE), jnp.float32)
        for w in range(4):
            count_rows = jnp.where(eight == w, count[w], count_rows)
            weight_rows = jnp.where(eight == w, count[w], weight_rows)

        squares[...] = jnp.zeros_like(squares)
        for which, ref in ((0, raw), (1, right)):
            for w in range(4):
                loads[4 * which + w].wait()
            means[which] = jnp.dot(live_rows, ref[pl.ds(0, tokens), :], preferred_element_type=jnp.float32)

        pl.semaphore_wait(barrier, 10)

        for which in (0, 1):
            stats[0, 0, me[0], which] = jnp.sum(means[which], axis=0, keepdims=True)
        stats[0, 0, me[0], 2] = jnp.full((1, width), device_count, jnp.float32)
        stat_start(0, 0)

        def to_means(j):
            cs = cs_of(j)
            for which in (0, 1):
                means[which, :, cs] = means[which, :, cs] / count_rows

        loop(width // LANE, to_means)

        def center(w):
            live = lax.broadcasted_iota(jnp.int32, (slots, LANE), 0) < counts_ref[w]
            lines = pl.ds(w * slots, slots)

            def centered_of(ref, which, cs):
                mean = means[which, w : w + 1, cs]
                x = jnp.where(live, ref[lines, cs].astype(jnp.float32) - mean, 0.0).astype(jnp.bfloat16)
                wide = x.astype(jnp.float32)
                squares[which, :, cs] += jnp.sum((wide * wide).reshape(slots // 8, 8, LANE), axis=0)
                return x

            def chunk(j):
                cs = cs_of(j)
                turned = centered_of(raw, 0, cs).T
                for k in range(groups):
                    left[core * half_blocks + j * groups + k, :, lines] = turned[k * block : (k + 1) * block]
                right[lines, cs] = centered_of(right, 1, cs)

            loop(width // LANE, chunk)
            window_push(w).start()

        center(0)
        stat_next(0, 0)
        center(1)
        stat_next(0, 1)
        center(2)
        stat_arrivals(0, 2)
        total = stat_sum(0, 2)
        for which in (0, 1):
            means_ref[which : which + 1, :] = total[which] / total[2]

        row16 = lax.broadcasted_iota(jnp.int32, (16, LANE), 0)

        def aux_rows(which, cs, weighted):
            grand = means_ref[which : which + 1, cs]
            packed = jnp.zeros((16, LANE), jnp.float32)
            for w in range(4):
                value = means[which, w : w + 1, cs] - grand
                if weighted:
                    value = count[w] * value
                high = value.astype(jnp.bfloat16).astype(jnp.float32)
                low = value - high
                order = (high, high, low, low) if weighted else (high, low, high, low)
                for k in range(4):
                    packed = jnp.where(row16 == 4 * k + w, order[k], packed)
            return jnp.concatenate([packed, jnp.zeros((AUX - 16, LANE), jnp.float32)], axis=0)

        def aux(j):
            cs = cs_of(j)
            turned = aux_rows(0, cs, True).T.astype(jnp.bfloat16)
            for k in range(groups):
                left[core * half_blocks + j * groups + k, :, pl.ds(tokens, AUX)] = turned[k * block : (k + 1) * block]
            right[pl.ds(tokens, AUX), cs] = aux_rows(1, cs, False).astype(jnp.bfloat16)

        loop(width // LANE, aux)
        aux_push().start()
        center(3)

        def spread(j):
            cs = cs_of(j)
            for which in (0, 1):
                shift = means[which, :, cs] - means_ref[which : which + 1, cs]
                part = squares[which, :, cs] + weight_rows * shift * shift
                stats[1, 0, me[0], which, :, cs] = jnp.sum(part, axis=0, keepdims=True)

        stats[1, 0, me[0], 2] = jnp.zeros((1, width), jnp.float32)
        loop(width // LANE, spread)
        stat_start(1, 0)

        for copy in pushes:
            copy.wait_recv()

    def reduce(acc):
        sums = acc.at[3]
        axes = [[lax.rem(core + q + k, 3) for k in range(3)] for q in range(3)]
        here = [[pick(axes[q][k], me) for k in range(3)] for q in range(3)]
        stride = [[pick(axes[q][k], (16, 4, 1)) for k in range(3)] for q in range(3)]

        def columns(q):
            return pl.ds(starts[q], widths[q])

        def moved(q, k, step):
            return lax.rem(here[q][k] + step, 4)

        def device(q, k, step):
            return at(axes[q][k], moved(q, k, step))

        def distance_of(k):
            return pick(k, DISTANCES)

        def multiply(q, first_step, second_step, into=None):
            base = moved(q, 0, first_step) * stride[q][0] + moved(q, 1, second_step) * stride[q][1]
            blocks = [left[base + moved(q, 2, distance) * stride[q][2]] for distance in DISTANCES]
            into = sums if into is None else into
            into[:, columns(q)] = jnp.dot(
                jnp.concatenate(blocks, axis=0), right[:, columns(q)], preferred_element_type=jnp.float32
            )

        def encoded(p, code_ref, scale_ref):
            peak = jnp.maximum(jnp.max(jnp.abs(p), axis=0, keepdims=True), 1e-30)
            code = jnp.round(p * (CODES / peak)).astype(jnp.int32)
            code_ref[...] = code.astype(jnp.int16)
            scale_ref[...] = peak * (1.0 / CODES)

        def encode_sums(q, code_ref, scale_ref):
            for cs in tiles(q):
                encoded(sums[:, cs], code_ref.at[:, cs], scale_ref.at[:, cs])

        def tiles(q):
            return [pl.ds(starts[q] + j, LANE) for j in range(0, widths[q], LANE)]

        def decoded(code_ref, scale_ref):
            return code_ref[...].astype(jnp.int32).astype(jnp.float32) * scale_ref[...]

        def each_tile(q, body):
            def step(j):
                body(pl.ds(pl.multiple_of(starts[q] + j * LANE, LANE), LANE))

            loop(widths[q] // LANE, step)

        def pair(code, code_to, scale, scale_to, sems, index, to):
            s, r, t, u = sems
            return (
                pltpu.make_async_remote_copy(
                    code, code_to, s.at[index], r.at[index], device_id=to, device_id_type=MESH
                ),
                pltpu.make_async_remote_copy(
                    scale, scale_to, t.at[index], u.at[index], device_id=to, device_id_type=MESH
                ),
            )

        far_sems = (far_s, far_r, far_t, far_u)
        near_sems = (near_s, near_r, near_t, near_u)
        mid_sems = (mid_s, mid_r, mid_t, mid_u)
        last_sems = (last_s, last_r, last_t, last_u)

        def far(q, k, way):
            cs = columns(q)
            lines = (upper, lower)[way]
            return pair(
                far_out.at[k, lines, cs], far_in.at[k, lines, cs],
                far_scale.at[k, :, cs], far_scale_in.at[2 * k + way, :, cs],
                far_sems, (q, 2 * k + way), device(q, 0, (1, 3)[way]),
            )

        def near(q, n, step):
            cs = columns(q)
            return pair(
                near_out.at[n, :, cs], near_in.at[n, :, cs], near_scale.at[n, :, cs], near_scale_in.at[n, :, cs],
                near_sems, (q, n), device(q, 0, step),
            )

        def start(copies):
            for copy in copies:
                copy.start()

        def arrived(copies):
            for copy in copies:
                copy.wait_recv()

        def gone(copies):
            for copy in copies:
                copy.wait_send()

        def serve_far(k):
            for q in range(3):
                if q < 2:
                    multiply(q + 1, 2, distance_of(k))
                else:
                    multiply(0, jnp.where(k == 3, 1, 2), pick(k, DISTANCES[1:] + DISTANCES[:1]))
                encode_sums(q, far_out.at[k], far_scale.at[k])
                start(far(q, k, 0))
                start(far(q, k, 1))

        def serve_near(k):
            for way in (0, 1):
                n = 2 * k + way
                for q in range(3):
                    arrived(far(q, k, way))
                    if q < 2:
                        multiply(q + 1, (1, 3)[way], distance_of(k))
                    elif way == 0:
                        multiply(0, 3, distance_of(k))
                    else:
                        multiply(0, jnp.where(k == 3, 0, 1), pick(k, DISTANCES[1:] + DISTANCES[3:]))
                    for cs in tiles(q):
                        p = sums[:, cs]
                        more = decoded(far_in.at[k, (upper, lower)[way], cs], far_scale_in.at[n, :, cs])
                        if way == 0:
                            p = jnp.concatenate([p[: rows // 2] + more, p[rows // 2 :]], axis=0)
                        else:
                            p = jnp.concatenate([p[: rows // 2], p[rows // 2 :] + more], axis=0)
                        encoded(p, near_out.at[n, :, cs], near_scale.at[n, :, cs])
                    start(near(q, n, (1, 3)[way]))

        multiply(0, 2, DISTANCES[0])
        loop(4, serve_far)
        stat_next(1, 0)
        def far_gone(k):
            for q in range(3):
                gone(far(q, k, 0))
                gone(far(q, k, 1))

        mid_out = far_out

        def mid(q, n, way=0):
            cs = columns(q)
            lines = (upper, lower)[way] if n == 0 else pl.ds(0, rows)
            k = way if n == 0 else n + 1
            step = (1, 3)[way] if n == 0 else (1, 3)[n - 1]
            return pair(
                mid_out.at[n, lines, cs], mid_in.at[n, lines, cs], mid_scale.at[n, :, cs], mid_scale_in.at[k, :, cs],
                mid_sems, (q, k), device(q, 1, step),
            )

        def merged(k, cs):
            n = 2 * k
            return (
                acc[k, :, cs]
                + decoded(near_in.at[n, :, cs], near_scale_in.at[n, :, cs])
                + decoded(near_in.at[n + 1, :, cs], near_scale_in.at[n + 1, :, cs])
            )

        def take_own(k):
            for q in range(3):
                arrived(near(q, 2 * k, 1))
                arrived(near(q, 2 * k + 1, 3))
                if k in (1, 2):
                    arrived(mid(q, 0, k - 1))

                def body(cs):
                    p = merged(k, cs)
                    if k == 3:
                        sums[:, cs] = p
                        return
                    if k == 1:
                        more = decoded(mid_in.at[0, upper, cs], mid_scale_in.at[0, :, cs])
                        p = jnp.concatenate([p[: rows // 2] + more, p[rows // 2 :]], axis=0)
                    if k == 2:
                        more = decoded(mid_in.at[0, lower, cs], mid_scale_in.at[1, :, cs])
                        p = jnp.concatenate([p[: rows // 2], p[rows // 2 :] + more], axis=0)
                    encoded(p, mid_out.at[k, :, cs], mid_scale.at[k, :, cs])

                each_tile(q, body)
                if k == 0:
                    start(mid(q, 0, 0))
                    start(mid(q, 0, 1))
                elif k < 3:
                    start(mid(q, k))

        def serve(k):
            serve_near(k)

            @pl.when(k == 0)
            def _():
                stat_next(1, 1)
                loop(4, far_gone)

            @pl.when(k >= 1)
            def _():
                for q in range(3):
                    multiply(q, 0, distance_of(k - 1), acc.at[k - 1])

            for before in range(3):

                @pl.when(k == before + 1)
                def _():
                    take_own(before)

        loop(4, serve)
        for q in (1, 2):
            multiply(q, 0, 0)
        take_own(3)
        stat_arrivals(1, 2)
        spread_first[core] = stat_sum(1, 2)
        spread_push = pltpu.make_async_remote_copy(
            spread_first.at[core], spread_first.at[core], peer_send.at[5], peer_recv.at[5],
            device_id=other, device_id_type=MESH,
        )
        spread_push.start()

        part = rows // 4
        half = part // 2
        front, back = pl.ds(0, half), pl.ds(half, half)

        def last(q, n, way=0):
            cs = columns(q)
            lines = (front, back)[way] if n == 0 else pl.ds(0, part)
            k = way if n == 0 else n + 1
            step = (1, 3)[way] if n == 0 else (1, 3)[n - 1]
            return pair(
                last_out.at[n, lines, cs], last_in.at[n, lines, cs], last_scale.at[n, :, cs], last_scale_in.at[k, :, cs],
                last_sems, (q, k), device(q, 2, step),
            )

        for q in range(3):
            arrived(mid(q, 1))
            arrived(mid(q, 2))

            def body(cs):
                p = (
                    sums[:, cs]
                    + decoded(mid_in.at[1, :, cs], mid_scale_in.at[2, :, cs])
                    + decoded(mid_in.at[2, :, cs], mid_scale_in.at[3, :, cs])
                )
                encoded(p[:part], last_out.at[0, :, cs], last_scale.at[0, :, cs])
                sums[pl.ds(part, 3 * part), cs] = p[part:]

            each_tile(q, body)
            start(last(q, 0, 0))
            start(last(q, 0, 1))

        for q in range(3):
            arrived(last(q, 0, 0))
            arrived(last(q, 0, 1))

            def body(cs):
                ahead = jnp.concatenate(
                    [
                        sums[pl.ds(part, half), cs] + decoded(last_in.at[0, front, cs], last_scale_in.at[0, :, cs]),
                        sums[pl.ds(part + half, half), cs],
                    ],
                    axis=0,
                )
                encoded(ahead, last_out.at[1, :, cs], last_scale.at[1, :, cs])
                behind = jnp.concatenate(
                    [
                        sums[pl.ds(2 * part, half), cs],
                        sums[pl.ds(2 * part + half, half), cs]
                        + decoded(last_in.at[0, back, cs], last_scale_in.at[1, :, cs]),
                    ],
                    axis=0,
                )
                encoded(behind, last_out.at[2, :, cs], last_scale.at[2, :, cs])

            each_tile(q, body)
            start(last(q, 1))
            start(last(q, 2))

        spread_push.wait_recv()
        grand_count = stat_sum(0, 2)[2, 0, 0]
        row_block = me[0] * 16 + me[1] * 4 + me[2]
        in_half = lax.rem(row_block, half_blocks)
        lane_block = cs_of(in_half * block // LANE)
        line = spread_first[row_block // half_blocks, 0, :, lane_block] / grand_count
        column[...] = jnp.broadcast_to(line, (LANE, LANE)).T
        rows_var = column[pl.ds(pl.multiple_of(lax.rem(in_half, groups) * block, block), block), :] + 0.1

        for q in range(3):
            arrived(last(q, 1))
            arrived(last(q, 2))

            def body(cs):
                cross = (
                    sums[pl.ds(3 * part, part), cs]
                    + decoded(last_in.at[1, :, cs], last_scale_in.at[2, :, cs])
                    + decoded(last_in.at[2, :, cs], last_scale_in.at[3, :, cs])
                )
                columns_var = spread_first[core, 1, :, cs] / grand_count + 0.1
                out_ref[:, cs] = cross / grand_count * lax.rsqrt(rows_var * columns_var)

            each_tile(q, body)

        def near_gone(k):
            for q in range(3):
                gone(near(q, 2 * k, 1))
                gone(near(q, 2 * k + 1, 3))

        loop(4, near_gone)
        for q in range(3):
            for copies in (mid, last):
                gone(copies(q, 0, 0))
                gone(copies(q, 0, 1))
                gone(copies(q, 1))
                gone(copies(q, 2))
        for copy in pushes + [spread_push]:
            copy.wait_send()
        for kind in (0, 1):
            for d in range(3):
                for copy in stat_copies(kind, d):
                    copy.wait_send()

    pl.run_scoped(prepare, pltpu.VMEM((tokens, width), jnp.bfloat16))
    pl.run_scoped(reduce, pltpu.VMEM((4, rows, width), jnp.float32))


def local(first_acts, second_acts, window_counts):
    tokens, width = first_acts.shape
    block = width * lax.axis_size("col") // lax.axis_size(TOK)
    blocks = width // block
    rows, depth = 4 * block, tokens + AUX
    i16, f32, bf16 = jnp.int16, jnp.float32, jnp.bfloat16
    dma = pltpu.SemaphoreType.DMA
    vmem = pltpu.VMEM
    return pl.pallas_call(
        functools.partial(kernel, widths_of(width)),
        out_shape=(jax.ShapeDtypeStruct((block, width), f32), jax.ShapeDtypeStruct((2, width), f32)),
        in_specs=[
            pl.BlockSpec(memory_space=pltpu.SMEM),
            pl.BlockSpec(memory_space=pl.ANY),
            pl.BlockSpec(memory_space=pl.ANY),
        ],
        out_specs=(pl.BlockSpec(memory_space=vmem), pl.BlockSpec(memory_space=vmem)),
        scratch_shapes=[
            vmem((2 * blocks, block, depth), bf16),
            vmem((depth, width), bf16),
            vmem((4, rows, width), i16), vmem((4, rows, width), i16),
            vmem((8, rows, width), i16), vmem((8, rows, width), i16),
            vmem((3, block, width), i16), vmem((3, block, width), i16),
            vmem((3, rows, width), i16),
            vmem((4, 1, width), f32), vmem((8, 1, width), f32),
            vmem((8, 1, width), f32), vmem((8, 1, width), f32),
            vmem((3, 1, width), f32), vmem((4, 1, width), f32),
            vmem((3, 1, width), f32), vmem((4, 1, width), f32),
            vmem((2, 8, width), f32), vmem((2, 8, width), f32),
            vmem((2, 3, 4, 3, 1, width), f32),
            vmem((2, 3, 1, width), f32),
            vmem((LANE, LANE), f32),
            dma((2, 4)), dma((6,)), dma((6,)),
            dma((3, 3)), dma((3, 4)), dma((3, 3)), dma((3, 4)),
            dma((3, 8)), dma((3, 8)), dma((3, 8)), dma((3, 8)),
            dma((3, 8)), dma((3, 8)), dma((3, 8)), dma((3, 8)),
            dma((3, 4)), dma((3, 4)), dma((3, 4)), dma((3, 4)),
            dma((3, 4)), dma((3, 4)), dma((3, 4)), dma((3, 4)),
        ],
        compiler_params=pltpu.CompilerParams(
            collective_id=0, has_side_effects=True, vmem_limit_bytes=67_043_328
        ),
        cost_estimate=pl.CostEstimate(
            flops=4 * width * width * depth, bytes_accessed=30_000_000, transcendentals=0
        ),
        name="whole",
    )(window_counts, first_acts, second_acts)


def solution(mesh):
    torus = Mesh(
        mesh.devices.reshape(4, 4, 4, mesh.shape["col"]), ("tok_0", "tok_1", "tok_2", "col")
    )
    return jax.shard_map(
        local,
        mesh=torus,
        in_specs=(P(TOK, "col"), P(TOK, "col"), P(TOK)),
        out_specs=(P(TOK, "col"), P(None, "col")),
        check_vma=False,
    )
```

```python
import functools

import jax
import jax.numpy as jnp
from jax import lax
from jax.experimental import pallas as pl
from jax.experimental.pallas import tpu as pltpu
from jax.sharding import Mesh
from jax.sharding import PartitionSpec as P

TOK = ("tok_0", "tok_1", "tok_2")
MESH = pl.DeviceIdType.MESH
LANE = 128
AUX = 128
CODES = 32767.0

DISTANCES = (2, 1, 3, 0)


def widths_of(width):
    tiles = width // LANE
    return [(tiles // 3 + (1 if q < tiles % 3 else 0)) * LANE for q in range(3)]


def pick(k, values):
    result = values[-1]
    for n in range(len(values) - 2, -1, -1):
        result = jnp.where(k == n, values[n], result)
    return result


def kernel(
    widths,
    counts_ref, first_hbm, second_hbm, out_ref,
    left, right, far_out, far_in, near_out, near_in, last_out, last_in, mid_in,
    far_scale, far_scale_in, near_scale, near_scale_in, mid_scale, mid_scale_in, last_scale, last_scale_in,
    sums_of, squares, rings, stats, spread_first, grand, column,
    load_sem, peer_send, peer_recv, ring_send, ring_recv, stat_send, stat_recv,
    far_s, far_r, far_t, far_u, near_s, near_r, near_t, near_u,
    mid_s, mid_r, mid_t, mid_u, last_s, last_r, last_t, last_u,
):
    me = [lax.axis_index(name) for name in TOK]
    core = lax.axis_index("col")
    width = right.shape[1]
    tokens = first_hbm.shape[0]
    depth = tokens + AUX
    slots = tokens // 4
    half_blocks = left.shape[0] // 2
    block = left.shape[1]
    starts = [sum(widths[:q]) for q in range(3)]
    rows = far_out.shape[1]
    upper, lower = pl.ds(0, rows // 2), pl.ds(rows // 2, rows // 2)

    def at(axis, coordinate):
        return {TOK[d]: jnp.where(axis == d, coordinate, me[d]) for d in range(3)}

    other = {"col": 1 - core}

    def cs_of(j):
        return pl.ds(pl.multiple_of(j * LANE, LANE), LANE)

    def loop(n, body):
        def step(j, _):
            body(j)
            return 0

        lax.fori_loop(0, n, step, 0)

    def exchange(ref, d, send, recv):
        for step in (1, 2, 3):
            pltpu.make_async_remote_copy(
                ref.at[me[d]], ref.at[me[d]], send, recv,
                device_id={TOK[d]: lax.rem(me[d] + step, 4)}, device_id_type=MESH,
            ).start()

    def exchanged(ref, d, send, recv):
        three = ref.at[pl.ds(0, 3)]
        return pltpu.make_async_remote_copy(
            three, three, send, recv, device_id={TOK[d]: lax.rem(me[d] + 1, 4)}, device_id_type=MESH
        )

    def ring(d):
        return rings.at[d], d, ring_send.at[d], ring_recv.at[d]

    def stat(kind, d):
        return stats.at[kind, d], d, stat_send.at[kind, d], stat_recv.at[kind, d]

    def added(ref):
        return ref[0] + ref[1] + ref[2] + ref[3]

    def stat_next(kind, d):
        now = ring(0) if (kind, d) == (0, 0) else stat(kind, d)
        exchanged(*now).wait_recv()
        stats[kind, d + 1, me[d + 1]] = added(now[0])
        exchange(*stat(kind, d + 1))

    mine = pl.ds(core * half_blocks, half_blocks)
    groups = LANE // block

    def push(lanes, k, half=mine):
        return pltpu.make_async_remote_copy(
            left.at[half, :, lanes], left.at[half, :, lanes], peer_send.at[k], peer_recv.at[k],
            device_id=other, device_id_type=MESH,
        )

    main_push = push(pl.ds(0, depth), 0)
    late_push = push(pl.ds(depth, AUX), 1)
    spread_push = pltpu.make_async_remote_copy(
        spread_first.at[core], spread_first.at[core], peer_send.at[2], peer_recv.at[2],
        device_id=other, device_id_type=MESH,
    )

    count = [counts_ref[w].astype(jnp.float32) for w in range(4)]
    device_count = count[0] + count[1] + count[2] + count[3]
    row16 = lax.broadcasted_iota(jnp.int32, (16, LANE), 0)

    def packed(values, weighted):
        result = jnp.zeros((16, LANE), jnp.float32)
        for w, value in enumerate(values):
            high = value.astype(jnp.bfloat16).astype(jnp.float32)
            low = value - high
            order = (high, high, low, low) if weighted else (high, low, high, low)
            for k in range(4):
                result = jnp.where(row16 == 4 * k + w, order[k], result)
        return result

    def put_left(j, lanes, rows):
        turned = rows.T.astype(jnp.bfloat16)
        for k in range(groups):
            left[core * half_blocks + j * groups + k, :, lanes] = turned[k * block : (k + 1) * block]

    def filled(rows):
        return jnp.concatenate([rows, jnp.zeros((AUX - rows.shape[0], LANE), jnp.float32)], axis=0)

    def prepare(raw):
        loads = []
        for w in range(4):
            lines = pl.ds(w * slots, slots)
            loads.append(pltpu.make_async_copy(first_hbm.at[lines], raw.at[lines], load_sem.at[0, w]))
        for w in range(4):
            lines = pl.ds(w * slots, slots)
            loads.append(pltpu.make_async_copy(second_hbm.at[lines], right.at[lines], load_sem.at[1, w]))
        for copy in loads:
            copy.start()
        barrier = pltpu.get_barrier_semaphore()
        for d in range(3):
            for step in (1, 2, 3):
                pl.semaphore_signal(
                    barrier, inc=1, device_id={TOK[d]: lax.rem(me[d] + step, 4)}, device_id_type=MESH
                )
        pl.semaphore_signal(barrier, inc=1, device_id=other, device_id_type=MESH)

        row = lax.broadcasted_iota(jnp.int32, (8, slots), 0)
        slot = lax.broadcasted_iota(jnp.int32, (8, slots), 1)
        squares[...] = jnp.zeros_like(squares)
        sums_of[...] = jnp.zeros_like(sums_of)

        def total_of(w):
            live = jnp.where((row == w) & (slot < counts_ref[w]), 1.0, 0.0).astype(jnp.bfloat16)
            for which, ref in ((0, raw), (1, right)):
                loads[4 * which + w].wait()
                sums_of[which] += jnp.dot(
                    live, ref[pl.ds(w * slots, slots), :], preferred_element_type=jnp.float32
                )

        def center(w):
            live = lax.broadcasted_iota(jnp.int32, (slots, LANE), 0) < counts_ref[w]
            lines = pl.ds(w * slots, slots)

            def centered_of(ref, which, cs):
                mean = sums_of[which, w : w + 1, cs] / count[w]
                x = jnp.where(live, ref[lines, cs].astype(jnp.float32) - mean, 0.0).astype(jnp.bfloat16)
                wide = x.astype(jnp.float32)
                squares[which, :, cs] += jnp.sum((wide * wide).reshape(slots // 8, 8, LANE), axis=0)
                return x

            def chunk(j):
                cs = cs_of(j)
                turned = centered_of(raw, 0, cs).T
                for k in range(groups):
                    left[core * half_blocks + j * groups + k, :, lines] = turned[k * block : (k + 1) * block]
                right[lines, cs] = centered_of(right, 1, cs)

            loop(width // LANE, chunk)
            push(lines, 0).start()

        total_of(0)
        pl.semaphore_wait(barrier, 10)
        center(0)
        for w in (1, 2):
            total_of(w)
            center(w)
        total_of(3)
        for which in (0, 1):
            device_sum = jnp.sum(sums_of[which], axis=0, keepdims=True)
            for d in range(3):
                rings[d, me[d], which] = device_sum
        for d in range(3):
            rings[d, me[d], 2] = jnp.full((1, width), device_count, jnp.float32)
        for d in range(3):
            exchange(*ring(d))

        def aux_rows(which, cs, weighted):
            device_mean = jnp.sum(sums_of[which, :, cs], axis=0, keepdims=True) / device_count
            values = []
            for w in range(4):
                value = sums_of[which, w : w + 1, cs] / count[w] - device_mean
                values.append(count[w] * value if weighted else value)
            return filled(packed(values, weighted))

        def aux(j):
            cs = cs_of(j)
            put_left(j, pl.ds(tokens, AUX), aux_rows(0, cs, True))
            right[pl.ds(tokens, AUX), cs] = aux_rows(1, cs, False).astype(jnp.bfloat16)

        loop(width // LANE, aux)
        push(pl.ds(tokens, AUX), 0).start()
        center(3)
        main_push.wait_recv()

    def reduce(acc):
        sums = acc.at[3]
        axes = [[lax.rem(core + q + k, 3) for k in range(3)] for q in range(3)]
        here = [[pick(axes[q][k], me) for k in range(3)] for q in range(3)]
        stride = [[pick(axes[q][k], (16, 4, 1)) for k in range(3)] for q in range(3)]

        def columns(q):
            return pl.ds(starts[q], widths[q])

        def moved(q, k, step):
            return lax.rem(here[q][k] + step, 4)

        def device(q, k, step):
            return at(axes[q][k], moved(q, k, step))

        def distance_of(k):
            return pick(k, DISTANCES)

        def multiply(q, first_step, second_step, into=None, lanes=depth):
            into = sums if into is None else into
            base = moved(q, 0, first_step) * stride[q][0] + moved(q, 1, second_step) * stride[q][1]
            deep = pl.ds(0, lanes)
            blocks = [left[base + moved(q, 2, distance) * stride[q][2], :, deep] for distance in DISTANCES]
            into[:, columns(q)] = jnp.dot(
                jnp.concatenate(blocks, axis=0), right[deep, columns(q)], preferred_element_type=jnp.float32
            )

        def multiply_own(q, second_step, into=None):
            multiply(q, 0, second_step, into, depth + AUX)

        def encoded(p, code_ref, scale_ref):
            peak = jnp.maximum(jnp.max(jnp.abs(p), axis=0, keepdims=True), 1e-30)
            code = jnp.round(p * (CODES / peak)).astype(jnp.int32)
            code_ref[...] = code.astype(jnp.int16)
            scale_ref[...] = peak * (1.0 / CODES)

        def encode_sums(q, code_ref, scale_ref):
            for cs in tiles(q):
                encoded(sums[:, cs], code_ref.at[:, cs], scale_ref.at[:, cs])

        def tiles(q):
            return [pl.ds(starts[q] + j, LANE) for j in range(0, widths[q], LANE)]

        def decoded(code_ref, scale_ref):
            return code_ref[...].astype(jnp.int32).astype(jnp.float32) * scale_ref[...]

        def each_tile(q, body):
            def step(j):
                body(pl.ds(pl.multiple_of(starts[q] + j * LANE, LANE), LANE))

            loop(widths[q] // LANE, step)

        def pair(code, code_to, scale, scale_to, sems, q, k, to):
            s, r, t, u = sems
            return (
                pltpu.make_async_remote_copy(
                    code, code_to, s.at[q], r.at[q, k], device_id=to, device_id_type=MESH
                ),
                pltpu.make_async_remote_copy(
                    scale, scale_to, t.at[q], u.at[q, k], device_id=to, device_id_type=MESH
                ),
            )

        far_sems = (far_s, far_r, far_t, far_u)
        near_sems = (near_s, near_r, near_t, near_u)
        mid_sems = (mid_s, mid_r, mid_t, mid_u)
        last_sems = (last_s, last_r, last_t, last_u)

        def far(q, k, way):
            cs = columns(q)
            lines = (upper, lower)[way]
            return pair(
                far_out.at[k, lines, cs], far_in.at[k, lines, cs],
                far_scale.at[k, :, cs], far_scale_in.at[2 * k + way, :, cs],
                far_sems, q, k, device(q, 0, (1, 3)[way]),
            )

        def near(q, n, step):
            cs = columns(q)
            return pair(
                near_out.at[n, :, cs], near_in.at[n, :, cs], near_scale.at[n, :, cs], near_scale_in.at[n, :, cs],
                near_sems, q, n // 2, device(q, 0, step),
            )

        def both(q, k, code, scale, lines, sems, axis):
            cs = columns(q)
            code, scale = code.at[lines[0], :, cs], scale.at[lines[1], :, cs]
            return pair(code, code, scale, scale, sems, q, k, device(q, axis, 1))

        def far_both(q, k):
            return both(q, k, far_in, far_scale_in, (pl.ds(k, 1), pl.ds(2 * k, 2)), far_sems, 0)

        def near_both(q, k):
            return both(q, k, near_in, near_scale_in, (pl.ds(2 * k, 2), pl.ds(2 * k, 2)), near_sems, 0)

        def mid_both(q, k):
            return both(q, k, mid_in, mid_scale_in, ((pl.ds(0, 1), pl.ds(1, 2))[k], pl.ds(2 * k, 2)), mid_sems, 1)

        def last_both(q, k):
            return both(q, k, last_in, last_scale_in, ((pl.ds(0, 1), pl.ds(1, 2))[k], pl.ds(2 * k, 2)), last_sems, 2)

        def far_all(q):
            return both(q, 0, far_in, far_scale_in, (pl.ds(0, 4), pl.ds(0, 8)), far_sems, 0)

        def near_all(q):
            return both(q, 0, near_in, near_scale_in, (pl.ds(0, 8), pl.ds(0, 8)), near_sems, 0)

        def mid_all(q):
            return both(q, 0, mid_in, mid_scale_in, (pl.ds(0, 3), pl.ds(0, 4)), mid_sems, 1)

        def last_all(q):
            return both(q, 0, last_in, last_scale_in, (pl.ds(0, 3), pl.ds(0, 4)), last_sems, 2)

        def start(copies):
            for copy in copies:
                copy.start()

        def arrived(copies):
            for copy in copies:
                copy.wait_recv()

        def gone(copies):
            for copy in copies:
                copy.wait_send()

        def serve_far(k):
            for q in range(3):
                if q < 2:
                    multiply(q + 1, 2, distance_of(k))
                else:
                    multiply(0, jnp.where(k == 3, 1, 2), pick(k, DISTANCES[1:] + DISTANCES[:1]))
                encode_sums(q, far_out.at[k], far_scale.at[k])
                start(far(q, k, 0))
                start(far(q, k, 1))

        def serve_near(k):
            for way in (0, 1):
                n = 2 * k + way
                for q in range(3):
                    if way == 0:
                        arrived(far_both(q, k))
                    if q < 2:
                        multiply(q + 1, (1, 3)[way], distance_of(k))
                    elif way == 0:
                        multiply(0, 3, distance_of(k))
                    else:
                        multiply(0, jnp.where(k == 3, 0, 1), pick(k, DISTANCES[1:] + DISTANCES[3:]))
                    for cs in tiles(q):
                        p = sums[:, cs]
                        more = decoded(far_in.at[k, (upper, lower)[way], cs], far_scale_in.at[n, :, cs])
                        if way == 0:
                            p = jnp.concatenate([p[: rows // 2] + more, p[rows // 2 :]], axis=0)
                        else:
                            p = jnp.concatenate([p[: rows // 2], p[rows // 2 :] + more], axis=0)
                        encoded(p, near_out.at[n, :, cs], near_scale.at[n, :, cs])
                    start(near(q, n, (1, 3)[way]))

        multiply(0, 2, DISTANCES[0])
        stat_next(0, 0)

        def serve_far_all(k):
            serve_far(k)

            @pl.when(k == 1)
            def _():
                stat_next(0, 1)

        loop(4, serve_far_all)

        exchanged(*stat(0, 2)).wait_recv()
        total = added(stats.at[0, 2])
        for which in (0, 1):
            grand[which : which + 1, :] = total[which] / total[2]
        grand_count = total[2, 0, 0]
        for d in (1, 2):
            exchanged(*ring(d)).wait_recv()

        def late_left(j):
            cs = cs_of(j)
            mean = grand[0:1, cs]
            rows = [
                packed([rings[d, m, 0, :, cs] - rings[d, m, 2, :, cs] * mean for m in range(4)], True) for d in range(3)
            ]
            put_left(j, pl.ds(depth, AUX), filled(jnp.concatenate(rows, axis=0)))

        loop(width // LANE, late_left)
        late_push.start()
        for q in range(3):
            d = axes[q][0]

            def late_right(cs):
                mean = grand[1:2, cs]
                rows = packed([rings[d, m, 1, :, cs] / rings[d, m, 2, :, cs] - mean for m in range(4)], False)
                rows = jnp.concatenate([jnp.where(d == k, rows, 0.0) for k in range(3)], axis=0)
                right[pl.ds(depth, AUX), cs] = filled(rows).astype(jnp.bfloat16)

            each_tile(q, late_right)

        eight = lax.broadcasted_iota(jnp.int32, (8, LANE), 0)
        weight_rows = jnp.zeros((8, LANE), jnp.float32)
        for w in range(4):
            weight_rows = jnp.where(eight == w, count[w], weight_rows)
        count_rows = jnp.maximum(weight_rows, 1.0)

        def spread(j):
            cs = cs_of(j)
            for which in (0, 1):
                shift = sums_of[which, :, cs] / count_rows - grand[which : which + 1, cs]
                part = squares[which, :, cs] + weight_rows * shift * shift
                stats[1, 0, me[0], which, :, cs] = jnp.sum(part, axis=0, keepdims=True)

        stats[1, 0, me[0], 2] = jnp.zeros((1, width), jnp.float32)
        loop(width // LANE, spread)
        exchange(*stat(1, 0))

        mid_out = far_out

        def mid(q, n, way=0):
            cs = columns(q)
            lines = (upper, lower)[way] if n == 0 else pl.ds(0, rows)
            k = way if n == 0 else n + 1
            step = (1, 3)[way] if n == 0 else (1, 3)[n - 1]
            return pair(
                mid_out.at[n, lines, cs], mid_in.at[n, lines, cs], mid_scale.at[n, :, cs], mid_scale_in.at[k, :, cs],
                mid_sems, q, k // 2, device(q, 1, step),
            )

        def merged(k, cs):
            n = 2 * k
            return (
                acc[k, :, cs]
                + decoded(near_in.at[n, :, cs], near_scale_in.at[n, :, cs])
                + decoded(near_in.at[n + 1, :, cs], near_scale_in.at[n + 1, :, cs])
            )

        def take_own(k):
            for q in range(3):
                arrived(near_both(q, k))
                if k == 1:
                    arrived(mid_both(q, 0))

                def body(cs):
                    p = merged(k, cs)
                    if k == 3:
                        sums[:, cs] = p
                        return
                    if k == 1:
                        more = decoded(mid_in.at[0, upper, cs], mid_scale_in.at[0, :, cs])
                        p = jnp.concatenate([p[: rows // 2] + more, p[rows // 2 :]], axis=0)
                    if k == 2:
                        more = decoded(mid_in.at[0, lower, cs], mid_scale_in.at[1, :, cs])
                        p = jnp.concatenate([p[: rows // 2], p[rows // 2 :] + more], axis=0)
                    encoded(p, mid_out.at[k, :, cs], mid_scale.at[k, :, cs])

                each_tile(q, body)
                if k == 0:
                    start(mid(q, 0, 0))
                    start(mid(q, 0, 1))
                elif k < 3:
                    start(mid(q, k))

        def serve(k):
            serve_near(k)

            @pl.when(k == 0)
            def _():
                stat_next(1, 0)
                late_push.wait_recv()

            @pl.when(k == 1)
            def _():
                stat_next(1, 1)
                for q in range(3):
                    gone(far_all(q))

            @pl.when(k >= 1)
            def _():
                for q in range(3):
                    multiply_own(q, distance_of(k - 1), acc.at[k - 1])

            for before in range(3):

                @pl.when(k == before + 1)
                def _():
                    take_own(before)

        loop(4, serve)
        for q in range(3):
            multiply_own(q, 0)
        take_own(3)
        exchanged(*stat(1, 2)).wait_recv()
        spread_first[core] = added(stats.at[1, 2])
        spread_push.start()

        part = rows // 4
        half = part // 2
        front, back = pl.ds(0, half), pl.ds(half, half)

        def last(q, n, way=0):
            cs = columns(q)
            lines = (front, back)[way] if n == 0 else pl.ds(0, part)
            k = way if n == 0 else n + 1
            step = (1, 3)[way] if n == 0 else (1, 3)[n - 1]
            return pair(
                last_out.at[n, lines, cs], last_in.at[n, lines, cs], last_scale.at[n, :, cs], last_scale_in.at[k, :, cs],
                last_sems, q, k // 2, device(q, 2, step),
            )

        for q in range(3):
            arrived(mid_both(q, 1))

            def body(cs):
                p = (
                    sums[:, cs]
                    + decoded(mid_in.at[1, :, cs], mid_scale_in.at[2, :, cs])
                    + decoded(mid_in.at[2, :, cs], mid_scale_in.at[3, :, cs])
                )
                encoded(p[:part], last_out.at[0, :, cs], last_scale.at[0, :, cs])
                sums[pl.ds(part, 3 * part), cs] = p[part:]

            each_tile(q, body)
            start(last(q, 0, 0))
            start(last(q, 0, 1))

        for q in range(3):
            arrived(last_both(q, 0))

            def body(cs):
                ahead = jnp.concatenate(
                    [
                        sums[pl.ds(part, half), cs] + decoded(last_in.at[0, front, cs], last_scale_in.at[0, :, cs]),
                        sums[pl.ds(part + half, half), cs],
                    ],
                    axis=0,
                )
                encoded(ahead, last_out.at[1, :, cs], last_scale.at[1, :, cs])
                behind = jnp.concatenate(
                    [
                        sums[pl.ds(2 * part, half), cs],
                        sums[pl.ds(2 * part + half, half), cs]
                        + decoded(last_in.at[0, back, cs], last_scale_in.at[1, :, cs]),
                    ],
                    axis=0,
                )
                encoded(behind, last_out.at[2, :, cs], last_scale.at[2, :, cs])

            each_tile(q, body)
            start(last(q, 1))
            start(last(q, 2))

        spread_push.wait_recv()
        row_block = me[0] * 16 + me[1] * 4 + me[2]
        in_half = lax.rem(row_block, half_blocks)
        lane_block = cs_of(in_half * block // LANE)
        line = spread_first[row_block // half_blocks, 0, :, lane_block] / grand_count
        column[...] = jnp.broadcast_to(line, (LANE, LANE)).T
        rows_var = column[pl.ds(pl.multiple_of(lax.rem(in_half, groups) * block, block), block), :] + 0.1

        for q in range(3):
            arrived(last_both(q, 1))

            def body(cs):
                cross = (
                    sums[pl.ds(3 * part, part), cs]
                    + decoded(last_in.at[1, :, cs], last_scale_in.at[2, :, cs])
                    + decoded(last_in.at[2, :, cs], last_scale_in.at[3, :, cs])
                )
                columns_var = spread_first[core, 1, :, cs] / grand_count + 0.1
                out_ref[pl.ds(0, block), cs] = cross / grand_count * lax.rsqrt(rows_var * columns_var)

            each_tile(q, body)

        out_ref[pl.ds(block, 2), :] = grand[0:2, :]

        for q in range(3):
            for copies in (near_all(q), mid_all(q), last_all(q)):
                gone(copies)
        for copy in (main_push, late_push, spread_push):
            copy.wait_send()
        for d in range(3):
            exchanged(*ring(d)).wait_send()
            exchanged(*stat(1, d)).wait_send()
            if d > 0:
                exchanged(*stat(0, d)).wait_send()

    pl.run_scoped(prepare, pltpu.VMEM((tokens, width), jnp.bfloat16))
    pl.run_scoped(reduce, pltpu.VMEM((4, rows, width), jnp.float32))


def local(first_acts, second_acts, window_counts):
    tokens, width = first_acts.shape
    block = width * lax.axis_size("col") // lax.axis_size(TOK)
    blocks = width // block
    rows, depth = 4 * block, tokens + 2 * AUX
    i16, f32, bf16 = jnp.int16, jnp.float32, jnp.bfloat16
    dma = pltpu.SemaphoreType.DMA
    vmem = pltpu.VMEM
    out = pl.pallas_call(
        functools.partial(kernel, widths_of(width)),
        out_shape=jax.ShapeDtypeStruct((block + 8, width), f32),
        in_specs=[
            pl.BlockSpec(memory_space=pltpu.SMEM),
            pl.BlockSpec(memory_space=pl.ANY),
            pl.BlockSpec(memory_space=pl.ANY),
        ],
        out_specs=pl.BlockSpec(memory_space=vmem),
        scratch_shapes=[
            vmem((2 * blocks, block, depth), bf16),
            vmem((depth, width), bf16),
            vmem((4, rows, width), i16), vmem((4, rows, width), i16),
            vmem((8, rows, width), i16), vmem((8, rows, width), i16),
            vmem((3, block, width), i16), vmem((3, block, width), i16),
            vmem((3, rows, width), i16),
            vmem((4, 1, width), f32), vmem((8, 1, width), f32),
            vmem((8, 1, width), f32), vmem((8, 1, width), f32),
            vmem((3, 1, width), f32), vmem((4, 1, width), f32),
            vmem((3, 1, width), f32), vmem((4, 1, width), f32),
            vmem((2, 8, width), f32), vmem((2, 8, width), f32),
            vmem((3, 4, 3, 1, width), f32),
            vmem((2, 3, 4, 3, 1, width), f32),
            vmem((2, 3, 1, width), f32),
            vmem((8, width), f32),
            vmem((LANE, LANE), f32),
            dma((2, 4)), dma((3,)), dma((3,)),
            dma((3,)), dma((3,)), dma((2, 3)), dma((2, 3)),
            dma((3,)), dma((3, 4)), dma((3,)), dma((3, 4)),
            dma((3,)), dma((3, 4)), dma((3,)), dma((3, 4)),
            dma((3,)), dma((3, 2)), dma((3,)), dma((3, 2)),
            dma((3,)), dma((3, 2)), dma((3,)), dma((3, 2)),
        ],
        compiler_params=pltpu.CompilerParams(
            collective_id=0, has_side_effects=True, vmem_limit_bytes=67_043_328
        ),
        cost_estimate=pl.CostEstimate(
            flops=4 * width * width * depth, bytes_accessed=30_000_000, transcendentals=0
        ),
        name="whole",
    )(window_counts, first_acts, second_acts)
    return out[:block], out[block : block + 2]


def solution(mesh):
    torus = Mesh(
        mesh.devices.reshape(4, 4, 4, mesh.shape["col"]), ("tok_0", "tok_1", "tok_2", "col")
    )
    return jax.shard_map(
        local,
        mesh=torus,
        in_specs=(P(TOK, "col"), P(TOK, "col"), P(TOK)),
        out_specs=(P(TOK, "col"), P(None, "col")),
        check_vma=False,
    )
```

```python
import functools

import jax
import jax.numpy as jnp
from jax import lax
from jax.experimental import pallas as pl
from jax.experimental.pallas import tpu as pltpu
from jax.sharding import Mesh
from jax.sharding import PartitionSpec as P

TOK = ("tok_0", "tok_1", "tok_2")
MESH = pl.DeviceIdType.MESH
LANE = 128
AUX = 128
CODES = 32767.0

DISTANCES = (2, 1, 3, 0)


def widths_of(width):
    tiles = width // LANE
    return [(tiles // 3 + (1 if q < tiles % 3 else 0)) * LANE for q in range(3)]


def pick(k, values):
    result = values[-1]
    for n in range(len(values) - 2, -1, -1):
        result = jnp.where(k == n, values[n], result)
    return result


def kernel(
    widths,
    counts_ref, first_hbm, second_hbm, out_ref,
    left, right, far_out, far_in, near_out, near_in, last_out, last_in, mid_in,
    far_scale, far_scale_in, near_scale, near_scale_in, mid_scale, mid_scale_in, last_scale, last_scale_in,
    sums_of, squares, rings, stats, spread_first, grand, column,
    load_sem, peer_send, peer_recv, ring_send, ring_recv, stat_send, stat_recv,
    far_s, far_r, far_t, far_u, near_s, near_r, near_t, near_u,
    mid_s, mid_r, mid_t, mid_u, last_s, last_r, last_t, last_u,
):
    me = [lax.axis_index(name) for name in TOK]
    core = lax.axis_index("col")
    width = right.shape[1]
    tokens = first_hbm.shape[0]
    depth = tokens + AUX
    slots = tokens // 4
    half_blocks = left.shape[0] // 2
    block = left.shape[1]
    starts = [sum(widths[:q]) for q in range(3)]
    rows = far_out.shape[1]
    upper, lower = pl.ds(0, rows // 2), pl.ds(rows // 2, rows // 2)

    def at(axis, coordinate):
        return {TOK[d]: jnp.where(axis == d, coordinate, me[d]) for d in range(3)}

    other = {"col": 1 - core}

    def cs_of(j):
        return pl.ds(pl.multiple_of(j * LANE, LANE), LANE)

    def loop(n, body):
        def step(j, _):
            body(j)
            return 0

        lax.fori_loop(0, n, step, 0)

    def loop_by(n, unroll, body):
        def step(j):
            for i in range(unroll):
                body(j * unroll + i)

        loop(n // unroll, step)

    def exchange(ref, d, send, recv):
        for step in (1, 2, 3):
            pltpu.make_async_remote_copy(
                ref.at[me[d]], ref.at[me[d]], send, recv,
                device_id={TOK[d]: lax.rem(me[d] + step, 4)}, device_id_type=MESH,
            ).start()

    def exchanged(ref, d, send, recv):
        three = ref.at[pl.ds(0, 3)]
        return pltpu.make_async_remote_copy(
            three, three, send, recv, device_id={TOK[d]: lax.rem(me[d] + 1, 4)}, device_id_type=MESH
        )

    def ring(d):
        return rings.at[d], d, ring_send.at[d], ring_recv.at[d]

    def stat(kind, d):
        return stats.at[kind, d], d, stat_send.at[kind, d], stat_recv.at[kind, d]

    def added(ref):
        return ref[0] + ref[1] + ref[2] + ref[3]

    def stat_next(kind, d):
        now = ring(0) if (kind, d) == (0, 0) else stat(kind, d)
        exchanged(*now).wait_recv()
        stats[kind, d + 1, me[d + 1]] = added(now[0])
        exchange(*stat(kind, d + 1))

    mine = pl.ds(core * half_blocks, half_blocks)
    groups = LANE // block

    def push(lanes, k, half=mine):
        return pltpu.make_async_remote_copy(
            left.at[half, :, lanes], left.at[half, :, lanes], peer_send.at[k], peer_recv.at[k],
            device_id=other, device_id_type=MESH,
        )

    main_push = push(pl.ds(0, depth), 0)
    late_push = push(pl.ds(depth, AUX), 1)
    spread_push = pltpu.make_async_remote_copy(
        spread_first.at[core], spread_first.at[core], peer_send.at[2], peer_recv.at[2],
        device_id=other, device_id_type=MESH,
    )

    count = [counts_ref[w].astype(jnp.float32) for w in range(4)]
    device_count = count[0] + count[1] + count[2] + count[3]
    row16 = lax.broadcasted_iota(jnp.int32, (16, LANE), 0)

    def packed(values, weighted):
        result = jnp.zeros((16, LANE), jnp.float32)
        for w, value in enumerate(values):
            high = value.astype(jnp.bfloat16).astype(jnp.float32)
            low = value - high
            order = (high, high, low, low) if weighted else (high, low, high, low)
            for k in range(4):
                result = jnp.where(row16 == 4 * k + w, order[k], result)
        return result

    def put_left(j, lanes, rows):
        turned = rows.T.astype(jnp.bfloat16)
        for k in range(groups):
            left[core * half_blocks + j * groups + k, :, lanes] = turned[k * block : (k + 1) * block]

    def filled(rows):
        return jnp.concatenate([rows, jnp.zeros((AUX - rows.shape[0], LANE), jnp.float32)], axis=0)

    def prepare(raw):
        loads = []
        for w in range(4):
            lines = pl.ds(w * slots, slots)
            loads.append(pltpu.make_async_copy(first_hbm.at[lines], raw.at[lines], load_sem.at[0, w]))
            loads.append(pltpu.make_async_copy(second_hbm.at[lines], right.at[lines], load_sem.at[1, w]))
        for copy in loads:
            copy.start()
        barrier = pltpu.get_barrier_semaphore()
        for d in range(3):
            for step in (1, 2, 3):
                pl.semaphore_signal(
                    barrier, inc=1, device_id={TOK[d]: lax.rem(me[d] + step, 4)}, device_id_type=MESH
                )
        pl.semaphore_signal(barrier, inc=1, device_id=other, device_id_type=MESH)

        row = lax.broadcasted_iota(jnp.int32, (8, slots), 0)
        slot = lax.broadcasted_iota(jnp.int32, (8, slots), 1)
        squares[...] = jnp.zeros_like(squares)
        sums_of[...] = jnp.zeros_like(sums_of)

        def total_of(w):
            live = jnp.where((row == w) & (slot < counts_ref[w]), 1.0, 0.0).astype(jnp.bfloat16)
            for which, ref in ((0, raw), (1, right)):
                loads[2 * w + which].wait()
                sums_of[which] += jnp.dot(
                    live, ref[pl.ds(w * slots, slots), :], preferred_element_type=jnp.float32
                )

        def center(w):
            live = lax.broadcasted_iota(jnp.int32, (slots, LANE), 0) < counts_ref[w]
            lines = pl.ds(w * slots, slots)

            def centered_of(ref, which, cs):
                mean = sums_of[which, w : w + 1, cs] / count[w]
                x = jnp.where(live, ref[lines, cs].astype(jnp.float32) - mean, 0.0).astype(jnp.bfloat16)
                wide = x.astype(jnp.float32)
                squares[which, :, cs] += jnp.sum((wide * wide).reshape(slots // 8, 8, LANE), axis=0)
                return x

            def chunk(j):
                cs = cs_of(j)
                turned = centered_of(raw, 0, cs).T
                for k in range(groups):
                    left[core * half_blocks + j * groups + k, :, lines] = turned[k * block : (k + 1) * block]
                right[lines, cs] = centered_of(right, 1, cs)

            pieces = 4 if w == 3 else 1
            chunks, step = width // LANE // pieces, half_blocks // pieces
            for piece in range(pieces):
                loop_by(chunks, 2, lambda j: chunk(piece * chunks + j))
                if w == 0:
                    pl.semaphore_wait(barrier, 10)
                push(lines, 0, pl.ds(core * half_blocks + piece * step, step)).start()

        total_of(0)
        center(0)
        for w in (1, 2):
            total_of(w)
            center(w)
        total_of(3)
        for which in (0, 1):
            device_sum = jnp.sum(sums_of[which], axis=0, keepdims=True)
            for d in range(3):
                rings[d, me[d], which] = device_sum
        for d in range(3):
            rings[d, me[d], 2] = jnp.full((1, width), device_count, jnp.float32)
        for d in range(3):
            exchange(*ring(d))

        def aux_rows(which, cs, weighted):
            device_mean = jnp.sum(sums_of[which, :, cs], axis=0, keepdims=True) / device_count
            values = []
            for w in range(4):
                value = sums_of[which, w : w + 1, cs] / count[w] - device_mean
                values.append(count[w] * value if weighted else value)
            return filled(packed(values, weighted))

        def aux(j):
            cs = cs_of(j)
            put_left(j, pl.ds(tokens, AUX), aux_rows(0, cs, True))
            right[pl.ds(tokens, AUX), cs] = aux_rows(1, cs, False).astype(jnp.bfloat16)

        loop_by(width // LANE, 4, aux)
        push(pl.ds(tokens, AUX), 0).start()
        center(3)
        main_push.wait_recv()

    def reduce(acc):
        sums = acc.at[3]
        axes = [[lax.rem(core + q + k, 3) for k in range(3)] for q in range(3)]
        here = [[pick(axes[q][k], me) for k in range(3)] for q in range(3)]
        stride = [[pick(axes[q][k], (16, 4, 1)) for k in range(3)] for q in range(3)]

        def columns(q):
            return pl.ds(starts[q], widths[q])

        def moved(q, k, step):
            return lax.rem(here[q][k] + step, 4)

        def device(q, k, step):
            return at(axes[q][k], moved(q, k, step))

        def distance_of(k):
            return pick(k, DISTANCES)

        def multiply(q, first_step, second_step, into=None, lanes=depth):
            into = sums if into is None else into
            base = moved(q, 0, first_step) * stride[q][0] + moved(q, 1, second_step) * stride[q][1]
            deep = pl.ds(0, lanes)
            blocks = [left[base + moved(q, 2, distance) * stride[q][2], :, deep] for distance in DISTANCES]
            into[:, columns(q)] = jnp.dot(
                jnp.concatenate(blocks, axis=0), right[deep, columns(q)], preferred_element_type=jnp.float32
            )

        def multiply_own(q, second_step, into=None):
            multiply(q, 0, second_step, into, depth + AUX)

        def encoded(p, code_ref, scale_ref):
            peak = jnp.maximum(jnp.max(jnp.abs(p), axis=0, keepdims=True), 1e-30)
            code = jnp.round(p * (CODES / peak)).astype(jnp.int32)
            code_ref[...] = code.astype(jnp.int16)
            scale_ref[...] = peak * (1.0 / CODES)

        def encode_sums(q, code_ref, scale_ref):
            for cs in tiles(q):
                encoded(sums[:, cs], code_ref.at[:, cs], scale_ref.at[:, cs])

        def tiles(q):
            return [pl.ds(starts[q] + j, LANE) for j in range(0, widths[q], LANE)]

        def decoded(code_ref, scale_ref):
            return code_ref[...].astype(jnp.int32).astype(jnp.float32) * scale_ref[...]

        def each_tile(q, body):
            def step(j):
                body(pl.ds(pl.multiple_of(starts[q] + j * LANE, LANE), LANE))

            loop(widths[q] // LANE, step)

        def pair(code, code_to, scale, scale_to, sems, q, k, to):
            s, r, t, u = sems
            return (
                pltpu.make_async_remote_copy(
                    code, code_to, s.at[q], r.at[q, k], device_id=to, device_id_type=MESH
                ),
                pltpu.make_async_remote_copy(
                    scale, scale_to, t.at[q], u.at[q, k], device_id=to, device_id_type=MESH
                ),
            )

        far_sems = (far_s, far_r, far_t, far_u)
        near_sems = (near_s, near_r, near_t, near_u)
        mid_sems = (mid_s, mid_r, mid_t, mid_u)
        last_sems = (last_s, last_r, last_t, last_u)

        def far(q, k, way):
            cs = columns(q)
            lines = (upper, lower)[way]
            return pair(
                far_out.at[k, lines, cs], far_in.at[k, lines, cs],
                far_scale.at[k, :, cs], far_scale_in.at[2 * k + way, :, cs],
                far_sems, q, k, device(q, 0, (1, 3)[way]),
            )

        def near(q, n, step):
            cs = columns(q)
            return pair(
                near_out.at[n, :, cs], near_in.at[n, :, cs], near_scale.at[n, :, cs], near_scale_in.at[n, :, cs],
                near_sems, q, n // 2, device(q, 0, step),
            )

        def both(q, k, code, scale, lines, sems, axis):
            cs = columns(q)
            code, scale = code.at[lines[0], :, cs], scale.at[lines[1], :, cs]
            return pair(code, code, scale, scale, sems, q, k, device(q, axis, 1))

        def far_both(q, k):
            return both(q, k, far_in, far_scale_in, (pl.ds(k, 1), pl.ds(2 * k, 2)), far_sems, 0)

        def near_both(q, k):
            return both(q, k, near_in, near_scale_in, (pl.ds(2 * k, 2), pl.ds(2 * k, 2)), near_sems, 0)

        def mid_both(q, k):
            return both(q, k, mid_in, mid_scale_in, ((pl.ds(0, 1), pl.ds(1, 2))[k], pl.ds(2 * k, 2)), mid_sems, 1)

        def last_both(q, k):
            return both(q, k, last_in, last_scale_in, ((pl.ds(0, 1), pl.ds(1, 2))[k], pl.ds(2 * k, 2)), last_sems, 2)

        def far_all(q):
            return both(q, 0, far_in, far_scale_in, (pl.ds(0, 4), pl.ds(0, 8)), far_sems, 0)

        def near_all(q):
            return both(q, 0, near_in, near_scale_in, (pl.ds(0, 8), pl.ds(0, 8)), near_sems, 0)

        def mid_all(q):
            return both(q, 0, mid_in, mid_scale_in, (pl.ds(0, 3), pl.ds(0, 4)), mid_sems, 1)

        def last_all(q):
            return both(q, 0, last_in, last_scale_in, (pl.ds(0, 3), pl.ds(0, 4)), last_sems, 2)

        def start(copies):
            for copy in copies:
                copy.start()

        def arrived(copies):
            for copy in copies:
                copy.wait_recv()

        def gone(copies):
            for copy in copies:
                copy.wait_send()

        def serve_far(k):
            for q in range(3):
                if q < 2:
                    multiply(q + 1, 2, distance_of(k))
                else:
                    multiply(0, jnp.where(k == 3, 1, 2), pick(k, DISTANCES[1:] + DISTANCES[:1]))
                encode_sums(q, far_out.at[k], far_scale.at[k])
            for q in range(3):
                start(far(q, k, 0))
                start(far(q, k, 1))

        def serve_near(k):
            for way in (0, 1):
                n = 2 * k + way
                if way == 0:
                    for q in range(3):
                        arrived(far_both(q, k))
                for q in range(3):
                    if q < 2:
                        multiply(q + 1, (1, 3)[way], distance_of(k))
                    elif way == 0:
                        multiply(0, 3, distance_of(k))
                    else:
                        multiply(0, jnp.where(k == 3, 0, 1), pick(k, DISTANCES[1:] + DISTANCES[3:]))
                    for cs in tiles(q):
                        p = sums[:, cs]
                        more = decoded(far_in.at[k, (upper, lower)[way], cs], far_scale_in.at[n, :, cs])
                        if way == 0:
                            p = jnp.concatenate([p[: rows // 2] + more, p[rows // 2 :]], axis=0)
                        else:
                            p = jnp.concatenate([p[: rows // 2], p[rows // 2 :] + more], axis=0)
                        encoded(p, near_out.at[n, :, cs], near_scale.at[n, :, cs])
                for q in range(3):
                    start(near(q, n, (1, 3)[way]))

        multiply(0, 2, DISTANCES[0])
        stat_next(0, 0)

        def serve_far_all(k):
            serve_far(k)

            @pl.when(k == 1)
            def _():
                stat_next(0, 1)

        loop(4, serve_far_all)

        def take_grand():
            exchanged(*stat(0, 2)).wait_recv()
            total = added(stats.at[0, 2])
            for which in (0, 1):
                grand[which : which + 1, :] = total[which] / total[2]
            for d in (1, 2):
                exchanged(*ring(d)).wait_recv()

            def late_left(j):
                cs = cs_of(j)
                mean = grand[0:1, cs]
                rows = [
                    packed([rings[d, m, 0, :, cs] - rings[d, m, 2, :, cs] * mean for m in range(4)], True) for d in range(3)
                ]
                put_left(j, pl.ds(depth, AUX), filled(jnp.concatenate(rows, axis=0)))

            loop_by(width // LANE, 4, late_left)
            late_push.start()
            for q in range(3):
                d = axes[q][0]

                def late_right(cs):
                    mean = grand[1:2, cs]
                    rows = packed([rings[d, m, 1, :, cs] / rings[d, m, 2, :, cs] - mean for m in range(4)], False)
                    rows = jnp.concatenate([jnp.where(d == k, rows, 0.0) for k in range(3)], axis=0)
                    right[pl.ds(depth, AUX), cs] = filled(rows).astype(jnp.bfloat16)

                each_tile(q, late_right)

            eight = lax.broadcasted_iota(jnp.int32, (8, LANE), 0)
            weight_rows = jnp.zeros((8, LANE), jnp.float32)
            for w in range(4):
                weight_rows = jnp.where(eight == w, count[w], weight_rows)
            count_rows = jnp.maximum(weight_rows, 1.0)

            def spread(j):
                cs = cs_of(j)
                for which in (0, 1):
                    shift = sums_of[which, :, cs] / count_rows - grand[which : which + 1, cs]
                    part = squares[which, :, cs] + weight_rows * shift * shift
                    stats[1, 0, me[0], which, :, cs] = jnp.sum(part, axis=0, keepdims=True)

            stats[1, 0, me[0], 2] = jnp.zeros((1, width), jnp.float32)
            loop(width // LANE, spread)
            exchange(*stat(1, 0))

        mid_out = far_out

        def mid(q, n, way=0):
            cs = columns(q)
            lines = (upper, lower)[way] if n == 0 else pl.ds(0, rows)
            k = way if n == 0 else n + 1
            step = (1, 3)[way] if n == 0 else (1, 3)[n - 1]
            return pair(
                mid_out.at[n, lines, cs], mid_in.at[n, lines, cs], mid_scale.at[n, :, cs], mid_scale_in.at[k, :, cs],
                mid_sems, q, k // 2, device(q, 1, step),
            )

        def merged(k, cs):
            n = 2 * k
            return (
                acc[k, :, cs]
                + decoded(near_in.at[n, :, cs], near_scale_in.at[n, :, cs])
                + decoded(near_in.at[n + 1, :, cs], near_scale_in.at[n + 1, :, cs])
            )

        def take_own(k, groups_of=(0, 1, 2)):
            for q in groups_of:
                arrived(near_both(q, k))
                if k == 1:
                    arrived(mid_both(q, 0))

                def body(cs):
                    p = merged(k, cs)
                    if k == 3:
                        sums[:, cs] = p
                        return
                    if k == 1:
                        more = decoded(mid_in.at[0, upper, cs], mid_scale_in.at[0, :, cs])
                        p = jnp.concatenate([p[: rows // 2] + more, p[rows // 2 :]], axis=0)
                    if k == 2:
                        more = decoded(mid_in.at[0, lower, cs], mid_scale_in.at[1, :, cs])
                        p = jnp.concatenate([p[: rows // 2], p[rows // 2 :] + more], axis=0)
                    encoded(p, mid_out.at[k, :, cs], mid_scale.at[k, :, cs])

                each_tile(q, body)
                if k == 0:
                    start(mid(q, 0, 0))
                    start(mid(q, 0, 1))
                elif k < 3:
                    start(mid(q, k))

        def serve(k):
            serve_near(k)

            @pl.when(k == 0)
            def _():
                take_grand()

            @pl.when(k == 1)
            def _():
                late_push.wait_recv()
                for q in range(3):
                    gone(far_all(q))

            @pl.when(k == 2)
            def _():
                stat_next(1, 0)

            @pl.when(k >= 1)
            def _():
                for q in range(3):
                    multiply_own(q, distance_of(k - 1), acc.at[k - 1])

            for before in range(3):

                @pl.when(k == before + 1)
                def _():
                    take_own(before)

        loop(4, serve)
        stat_next(1, 1)
        for q in range(3):
            multiply_own(q, 0)

        part = rows // 4
        half = part // 2
        front, back = pl.ds(0, half), pl.ds(half, half)

        def last(q, n, way=0):
            cs = columns(q)
            lines = (front, back)[way] if n == 0 else pl.ds(0, part)
            k = way if n == 0 else n + 1
            step = (1, 3)[way] if n == 0 else (1, 3)[n - 1]
            return pair(
                last_out.at[n, lines, cs], last_in.at[n, lines, cs], last_scale.at[n, :, cs], last_scale_in.at[k, :, cs],
                last_sems, q, k // 2, device(q, 2, step),
            )

        for q in range(3):
            take_own(3, (q,))
            arrived(mid_both(q, 1))

            def body(cs):
                p = (
                    sums[:, cs]
                    + decoded(mid_in.at[1, :, cs], mid_scale_in.at[2, :, cs])
                    + decoded(mid_in.at[2, :, cs], mid_scale_in.at[3, :, cs])
                )
                encoded(p[:part], last_out.at[0, :, cs], last_scale.at[0, :, cs])
                sums[pl.ds(part, 3 * part), cs] = p[part:]

            each_tile(q, body)
            start(last(q, 0, 0))
            start(last(q, 0, 1))

        exchanged(*stat(1, 2)).wait_recv()
        spread_first[core] = added(stats.at[1, 2])
        spread_push.start()
        for q in range(3):
            arrived(last_both(q, 0))

            def body(cs):
                ahead = jnp.concatenate(
                    [
                        sums[pl.ds(part, half), cs] + decoded(last_in.at[0, front, cs], last_scale_in.at[0, :, cs]),
                        sums[pl.ds(part + half, half), cs],
                    ],
                    axis=0,
                )
                encoded(ahead, last_out.at[1, :, cs], last_scale.at[1, :, cs])
                behind = jnp.concatenate(
                    [
                        sums[pl.ds(2 * part, half), cs],
                        sums[pl.ds(2 * part + half, half), cs]
                        + decoded(last_in.at[0, back, cs], last_scale_in.at[1, :, cs]),
                    ],
                    axis=0,
                )
                encoded(behind, last_out.at[2, :, cs], last_scale.at[2, :, cs])

            each_tile(q, body)
            start(last(q, 1))
            start(last(q, 2))

        spread_push.wait_recv()
        grand_count = added(stats.at[0, 2])[2, 0, 0]
        row_block = me[0] * 16 + me[1] * 4 + me[2]
        in_half = lax.rem(row_block, half_blocks)
        lane_block = cs_of(in_half * block // LANE)
        line = spread_first[row_block // half_blocks, 0, :, lane_block] / grand_count
        column[...] = jnp.broadcast_to(line, (LANE, LANE)).T
        rows_var = column[pl.ds(pl.multiple_of(lax.rem(in_half, groups) * block, block), block), :] + 0.1

        for q in range(3):
            arrived(last_both(q, 1))

            def body(cs):
                cross = (
                    sums[pl.ds(3 * part, part), cs]
                    + decoded(last_in.at[1, :, cs], last_scale_in.at[2, :, cs])
                    + decoded(last_in.at[2, :, cs], last_scale_in.at[3, :, cs])
                )
                columns_var = spread_first[core, 1, :, cs] / grand_count + 0.1
                out_ref[pl.ds(0, block), cs] = cross / grand_count * lax.rsqrt(rows_var * columns_var)

            each_tile(q, body)

        out_ref[pl.ds(block, 2), :] = grand[0:2, :]

        for q in range(3):
            for copies in (near_all(q), mid_all(q), last_all(q)):
                gone(copies)
        for copy in (main_push, late_push, spread_push):
            copy.wait_send()
        for d in range(3):
            exchanged(*ring(d)).wait_send()
            exchanged(*stat(1, d)).wait_send()
            if d > 0:
                exchanged(*stat(0, d)).wait_send()

    pl.run_scoped(prepare, pltpu.VMEM((tokens, width), jnp.bfloat16))
    pl.run_scoped(reduce, pltpu.VMEM((4, rows, width), jnp.float32))


def local(first_acts, second_acts, window_counts):
    tokens, width = first_acts.shape
    block = width * lax.axis_size("col") // lax.axis_size(TOK)
    blocks = width // block
    rows, depth = 4 * block, tokens + 2 * AUX
    i16, f32, bf16 = jnp.int16, jnp.float32, jnp.bfloat16
    dma = pltpu.SemaphoreType.DMA
    vmem = pltpu.VMEM
    out = pl.pallas_call(
        functools.partial(kernel, widths_of(width)),
        out_shape=jax.ShapeDtypeStruct((block + 8, width), f32),
        in_specs=[
            pl.BlockSpec(memory_space=pltpu.SMEM),
            pl.BlockSpec(memory_space=pl.ANY),
            pl.BlockSpec(memory_space=pl.ANY),
        ],
        out_specs=pl.BlockSpec(memory_space=vmem),
        scratch_shapes=[
            vmem((2 * blocks, block, depth), bf16),
            vmem((depth, width), bf16),
            vmem((4, rows, width), i16), vmem((4, rows, width), i16),
            vmem((8, rows, width), i16), vmem((8, rows, width), i16),
            vmem((3, block, width), i16), vmem((3, block, width), i16),
            vmem((3, rows, width), i16),
            vmem((4, 1, width), f32), vmem((8, 1, width), f32),
            vmem((8, 1, width), f32), vmem((8, 1, width), f32),
            vmem((3, 1, width), f32), vmem((4, 1, width), f32),
            vmem((3, 1, width), f32), vmem((4, 1, width), f32),
            vmem((2, 8, width), f32), vmem((2, 8, width), f32),
            vmem((3, 4, 3, 1, width), f32),
            vmem((2, 3, 4, 3, 1, width), f32),
            vmem((2, 3, 1, width), f32),
            vmem((8, width), f32),
            vmem((LANE, LANE), f32),
            dma((2, 4)), dma((3,)), dma((3,)),
            dma((3,)), dma((3,)), dma((2, 3)), dma((2, 3)),
            dma((3,)), dma((3, 4)), dma((3,)), dma((3, 4)),
            dma((3,)), dma((3, 4)), dma((3,)), dma((3, 4)),
            dma((3,)), dma((3, 2)), dma((3,)), dma((3, 2)),
            dma((3,)), dma((3, 2)), dma((3,)), dma((3, 2)),
        ],
        compiler_params=pltpu.CompilerParams(
            collective_id=0, has_side_effects=True, vmem_limit_bytes=67_043_328
        ),
        cost_estimate=pl.CostEstimate(
            flops=4 * width * width * depth, bytes_accessed=30_000_000, transcendentals=0
        ),
        name="whole",
    )(window_counts, first_acts, second_acts)
    return out[:block], out[block : block + 2]


def solution(mesh):
    torus = Mesh(
        mesh.devices.reshape(4, 4, 4, mesh.shape["col"]), ("tok_0", "tok_1", "tok_2", "col")
    )
    return jax.shard_map(
        local,
        mesh=torus,
        in_specs=(P(TOK, "col"), P(TOK, "col"), P(TOK)),
        out_specs=(P(TOK, "col"), P(None, "col")),
        check_vma=False,
    )
```

```python
import functools

import jax
import jax.numpy as jnp
from jax import lax
from jax.experimental import pallas as pl
from jax.experimental.pallas import tpu as pltpu
from jax.sharding import Mesh
from jax.sharding import PartitionSpec as P

TOK = ("tok_0", "tok_1", "tok_2")
MESH = pl.DeviceIdType.MESH
LANE = 128
AUX = 128
CODES = 32767.0

DISTANCES = (2, 1, 3, 0)


def widths_of(width):
    tiles = width // LANE
    return [(tiles // 3 + (1 if q < tiles % 3 else 0)) * LANE for q in range(3)]


def pick(k, values):
    result = values[-1]
    for n in range(len(values) - 2, -1, -1):
        result = jnp.where(k == n, values[n], result)
    return result


def kernel(
    widths,
    counts_ref, first_hbm, second_hbm, out_ref,
    left, right, far_out, far_in, near_out, near_in, last_out, last_in, mid_in,
    far_scale, far_scale_in, near_scale, near_scale_in, mid_scale, mid_scale_in, last_scale, last_scale_in,
    sums_of, squares, live_slots, rings, stats, spread_first, grand, column,
    load_sem, peer_send, peer_recv, ring_send, ring_recv, stat_send, stat_recv,
    far_s, far_r, far_t, far_u, near_s, near_r, near_t, near_u,
    mid_s, mid_r, mid_t, mid_u, last_s, last_r, last_t, last_u,
):
    me = [lax.axis_index(name) for name in TOK]
    core = lax.axis_index("col")
    width = right.shape[1]
    tokens = first_hbm.shape[0]
    depth = tokens + AUX
    slots = tokens // 4
    half_blocks = left.shape[0] // 2
    block = left.shape[1]
    starts = [sum(widths[:q]) for q in range(3)]
    rows = far_out.shape[1]
    upper, lower = pl.ds(0, rows // 2), pl.ds(rows // 2, rows // 2)

    def at(axis, coordinate):
        return {TOK[d]: jnp.where(axis == d, coordinate, me[d]) for d in range(3)}

    other = {"col": 1 - core}

    tail = pl.ds(width, LANE)

    def cs_of(j):
        return pl.ds(pl.multiple_of(j * LANE, LANE), LANE)

    def loop(n, body):
        def step(j, _):
            body(j)
            return 0

        lax.fori_loop(0, n, step, 0)

    def loop_by(n, unroll, body):
        def step(j):
            for i in range(unroll):
                body(j * unroll + i)

        loop(n // unroll, step)

    def exchange(ref, d, send, recv):
        for step in (1, 2, 3):
            pltpu.make_async_remote_copy(
                ref.at[me[d]], ref.at[me[d]], send, recv,
                device_id={TOK[d]: lax.rem(me[d] + step, 4)}, device_id_type=MESH,
            ).start()

    def exchanged(ref, d, send, recv):
        three = ref.at[pl.ds(0, 3)]
        return pltpu.make_async_remote_copy(
            three, three, send, recv, device_id={TOK[d]: lax.rem(me[d] + 1, 4)}, device_id_type=MESH
        )

    def ring(d):
        return rings.at[d], d, ring_send.at[d], ring_recv.at[d]

    def stat(kind, d):
        return stats.at[kind, d], d, stat_send.at[kind, d], stat_recv.at[kind, d]

    def added(ref):
        return ref[0] + ref[1] + ref[2] + ref[3]

    def stat_next(kind, d):
        now = ring(0) if (kind, d) == (0, 0) else stat(kind, d)
        exchanged(*now).wait_recv()
        stats[kind, d + 1, me[d + 1]] = added(now[0])
        exchange(*stat(kind, d + 1))

    mine = pl.ds(core * half_blocks, half_blocks)
    groups = LANE // block

    def push(lanes, k, half=mine):
        return pltpu.make_async_remote_copy(
            left.at[half, :, lanes], left.at[half, :, lanes], peer_send.at[k], peer_recv.at[k],
            device_id=other, device_id_type=MESH,
        )

    main_push = push(pl.ds(0, depth), 0)
    late_push = push(pl.ds(depth, AUX), 1)
    spread_push = pltpu.make_async_remote_copy(
        spread_first.at[core], spread_first.at[core], peer_send.at[2], peer_recv.at[2],
        device_id=other, device_id_type=MESH,
    )

    count = [counts_ref[w].astype(jnp.float32) for w in range(4)]
    device_count = count[0] + count[1] + count[2] + count[3]
    row16 = lax.broadcasted_iota(jnp.int32, (16, LANE), 0)

    def packed(values, weighted):
        result = jnp.zeros((16, LANE), jnp.float32)
        for w, value in enumerate(values):
            high = value.astype(jnp.bfloat16).astype(jnp.float32)
            low = value - high
            order = (high, high, low, low) if weighted else (high, low, high, low)
            for k in range(4):
                result = jnp.where(row16 == 4 * k + w, order[k], result)
        return result

    def put_left(j, lanes, rows):
        turned = rows.T.astype(jnp.bfloat16)
        for k in range(groups):
            left[core * half_blocks + j * groups + k, :, lanes] = turned[k * block : (k + 1) * block]

    def filled(rows):
        return jnp.concatenate([rows, jnp.zeros((AUX - rows.shape[0], LANE), jnp.float32)], axis=0)

    def prepare(raw):
        loads = []
        for w in range(4):
            lines = pl.ds(w * slots, slots)
            loads.append(pltpu.make_async_copy(first_hbm.at[lines], raw.at[lines], load_sem.at[0, w]))
            loads.append(pltpu.make_async_copy(second_hbm.at[lines], right.at[lines], load_sem.at[1, w]))
        for copy in loads:
            copy.start()
        barrier = pltpu.get_barrier_semaphore()
        for d in range(3):
            for step in (1, 2, 3):
                pl.semaphore_signal(
                    barrier, inc=1, device_id={TOK[d]: lax.rem(me[d] + step, 4)}, device_id_type=MESH
                )
        pl.semaphore_signal(barrier, inc=1, device_id=other, device_id_type=MESH)

        row = lax.broadcasted_iota(jnp.int32, (8, slots), 0)
        slot = lax.broadcasted_iota(jnp.int32, (8, slots), 1)
        squares[...] = jnp.zeros_like(squares)
        sums_of[...] = jnp.zeros_like(sums_of)

        def total_of(w):
            live = jnp.where((row == w) & (slot < counts_ref[w]), 1.0, 0.0).astype(jnp.bfloat16)
            for which, ref in ((0, raw), (1, right)):
                loads[2 * w + which].wait()
                sums_of[which] += jnp.dot(
                    live, ref[pl.ds(w * slots, slots), :], preferred_element_type=jnp.float32
                )

        def center(w):
            live = lax.broadcasted_iota(jnp.int32, (slots, LANE), 0) < counts_ref[w]
            live_slots[...] = jnp.where(live, 1.0, 0.0).astype(jnp.bfloat16)
            lines = pl.ds(w * slots, slots)

            def centered_of(ref, which, cs):
                mean = sums_of[which, w : w + 1, cs] / count[w]
                x = (ref[lines, cs].astype(jnp.float32) - mean).astype(jnp.bfloat16) * live_slots[...]
                wide = x.astype(jnp.float32)
                squares[which, :, cs] += jnp.sum((wide * wide).reshape(slots // 8, 8, LANE), axis=0)
                return x

            def chunk(j):
                cs = cs_of(j)
                turned = centered_of(raw, 0, cs).T
                for k in range(groups):
                    left[core * half_blocks + j * groups + k, :, lines] = turned[k * block : (k + 1) * block]
                right[lines, cs] = centered_of(right, 1, cs)

            pieces = (1, 2, 2, 4)[w]
            chunks, step = width // LANE // pieces, half_blocks // pieces
            for piece in range(pieces):
                loop_by(chunks, 2, lambda j: chunk(piece * chunks + j))
                if w == 0:
                    pl.semaphore_wait(barrier, 10)
                push(lines, 0, pl.ds(core * half_blocks + piece * step, step)).start()

        total_of(0)
        center(0)
        for w in (1, 2):
            total_of(w)
            center(w)
        total_of(3)
        for which in (0, 1):
            device_sum = jnp.sum(sums_of[which], axis=0, keepdims=True)
            for d in range(3):
                rings[d, me[d], which, :, pl.ds(0, width)] = device_sum
                rings[d, me[d], which, :, tail] = jnp.full((1, LANE), device_count, jnp.float32)
        for d in range(3):
            exchange(*ring(d))

        def aux_rows(which, cs, weighted):
            device_mean = jnp.sum(sums_of[which, :, cs], axis=0, keepdims=True) / device_count
            values = []
            for w in range(4):
                value = sums_of[which, w : w + 1, cs] / count[w] - device_mean
                values.append(count[w] * value if weighted else value)
            return filled(packed(values, weighted))

        def aux(j):
            cs = cs_of(j)
            put_left(j, pl.ds(tokens, AUX), aux_rows(0, cs, True))
            right[pl.ds(tokens, AUX), cs] = aux_rows(1, cs, False).astype(jnp.bfloat16)

        loop_by(width // LANE, 4, aux)
        push(pl.ds(tokens, AUX), 0).start()
        center(3)
        main_push.wait_recv()

    def reduce(acc):
        sums = acc.at[3]
        axes = [[lax.rem(core + q + k, 3) for k in range(3)] for q in range(3)]
        here = [[pick(axes[q][k], me) for k in range(3)] for q in range(3)]
        stride = [[pick(axes[q][k], (16, 4, 1)) for k in range(3)] for q in range(3)]

        def columns(q):
            return pl.ds(starts[q], widths[q])

        def moved(q, k, step):
            return lax.rem(here[q][k] + step, 4)

        def device(q, k, step):
            return at(axes[q][k], moved(q, k, step))

        def distance_of(k):
            return pick(k, DISTANCES)

        def multiply(q, first_step, second_step, into=None, lanes=depth):
            into = sums if into is None else into
            base = moved(q, 0, first_step) * stride[q][0] + moved(q, 1, second_step) * stride[q][1]
            deep = pl.ds(0, lanes)
            blocks = [left[base + moved(q, 2, distance) * stride[q][2], :, deep] for distance in DISTANCES]
            into[:, columns(q)] = jnp.dot(
                jnp.concatenate(blocks, axis=0), right[deep, columns(q)], preferred_element_type=jnp.float32
            )

        def multiply_own(q, second_step, into=None):
            multiply(q, 0, second_step, into, depth + AUX)

        def encoded(p, code_ref, scale_ref):
            peak = jnp.maximum(jnp.max(jnp.abs(p), axis=0, keepdims=True), 1e-30)
            code = jnp.round(p * (CODES / peak)).astype(jnp.int32)
            code_ref[...] = code.astype(jnp.int16)
            scale_ref[...] = peak * (1.0 / CODES)

        def encode_sums(q, code_ref, scale_ref):
            for cs in tiles(q):
                encoded(sums[:, cs], code_ref.at[:, cs], scale_ref.at[:, cs])

        def tiles(q):
            return [pl.ds(starts[q] + j, LANE) for j in range(0, widths[q], LANE)]

        def decoded(code_ref, scale_ref):
            return code_ref[...].astype(jnp.int32).astype(jnp.float32) * scale_ref[...]

        def each_tile(q, body):
            def step(j):
                body(pl.ds(pl.multiple_of(starts[q] + j * LANE, LANE), LANE))

            loop(widths[q] // LANE, step)

        def pair(code, code_to, scale, scale_to, sems, q, k, to):
            s, r, t, u = sems
            return (
                pltpu.make_async_remote_copy(
                    code, code_to, s.at[0], r.at[q, k], device_id=to, device_id_type=MESH
                ),
                pltpu.make_async_remote_copy(
                    scale, scale_to, t.at[0], u.at[q, k], device_id=to, device_id_type=MESH
                ),
            )

        far_sems = (far_s, far_r, far_t, far_u)
        near_sems = (near_s, near_r, near_t, near_u)
        mid_sems = (mid_s, mid_r, mid_t, mid_u)
        last_sems = (last_s, last_r, last_t, last_u)

        def far(q, k, way):
            cs = columns(q)
            lines = (upper, lower)[way]
            return pair(
                far_out.at[k, lines, cs], far_in.at[k, lines, cs],
                far_scale.at[k, :, cs], far_scale_in.at[2 * k + way, :, cs],
                far_sems, 0, k, device(q, 0, (1, 3)[way]),
            )

        def near(q, n, step):
            cs = columns(q)
            return pair(
                near_out.at[n, :, cs], near_in.at[n, :, cs], near_scale.at[n, :, cs], near_scale_in.at[n, :, cs],
                near_sems, q, n // 2, device(q, 0, step),
            )

        def both(q, k, code, scale, lines, sems, axis):
            cs = pl.ds(0, width) if q is None else columns(q)
            q = 0 if q is None else q
            code, scale = code.at[lines[0], :, cs], scale.at[lines[1], :, cs]
            return pair(code, code, scale, scale, sems, q, k, device(q, axis, 1))

        def far_both(k):
            return both(None, k, far_in, far_scale_in, (pl.ds(k, 1), pl.ds(2 * k, 2)), far_sems, 0)

        def near_both(q, k):
            return both(q, k, near_in, near_scale_in, (pl.ds(2 * k, 2), pl.ds(2 * k, 2)), near_sems, 0)

        def mid_both(q, k):
            return both(q, k, mid_in, mid_scale_in, ((pl.ds(0, 1), pl.ds(1, 2))[k], pl.ds(2 * k, 2)), mid_sems, 1)

        def last_both(q, k):
            return both(q, k, last_in, last_scale_in, ((pl.ds(0, 1), pl.ds(1, 2))[k], (pl.ds(0, 2), pl.ds(2, 4))[k]), last_sems, 2)

        def far_all():
            return both(None, 0, far_in, far_scale_in, (pl.ds(0, 4), pl.ds(0, 8)), far_sems, 0)

        def near_all():
            return both(None, 0, near_in, near_scale_in, (pl.ds(0, 8), pl.ds(0, 8)), near_sems, 0)

        def mid_all():
            return both(None, 0, mid_in, mid_scale_in, (pl.ds(0, 3), pl.ds(0, 4)), mid_sems, 1)

        def last_all():
            return both(None, 0, last_in, last_scale_in, (pl.ds(0, 3), pl.ds(0, 6)), last_sems, 2)

        def start(copies):
            for copy in copies:
                copy.start()

        def arrived(copies):
            for copy in copies:
                copy.wait_recv()

        def gone(copies):
            for copy in copies:
                copy.wait_send()

        def serve_far(k):
            for q in range(3):
                if q < 2:
                    multiply(q + 1, 2, distance_of(k))
                else:
                    multiply(0, jnp.where(k == 3, 1, 2), pick(k, DISTANCES[1:] + DISTANCES[:1]))
                encode_sums(q, far_out.at[k], far_scale.at[k])
            for q in range(3):
                start(far(q, k, 0))
                start(far(q, k, 1))

        def serve_near(k):
            for way in (0, 1):
                n = 2 * k + way
                if way == 0:
                    arrived(far_both(k))
                for q in range(3):
                    if q < 2:
                        multiply(q + 1, (1, 3)[way], distance_of(k))
                    elif way == 0:
                        multiply(0, 3, distance_of(k))
                    else:
                        multiply(0, jnp.where(k == 3, 0, 1), pick(k, DISTANCES[1:] + DISTANCES[3:]))
                    for cs in tiles(q):
                        p = sums[:, cs]
                        more = decoded(far_in.at[k, (upper, lower)[way], cs], far_scale_in.at[n, :, cs])
                        if way == 0:
                            p = jnp.concatenate([p[: rows // 2] + more, p[rows // 2 :]], axis=0)
                        else:
                            p = jnp.concatenate([p[: rows // 2], p[rows // 2 :] + more], axis=0)
                        encoded(p, near_out.at[n, :, cs], near_scale.at[n, :, cs])
                for q in range(3):
                    start(near(q, n, (1, 3)[way]))

        multiply(0, 2, DISTANCES[0])
        for q in range(3):
            if q < 2:
                multiply(q + 1, 2, DISTANCES[0])
            else:
                multiply(0, 2, DISTANCES[1])
            encode_sums(q, far_out.at[0], far_scale.at[0])
            start(far(q, 0, 0))
            start(far(q, 0, 1))
        stat_next(0, 0)

        def serve_far_all(k):
            serve_far(k)

            @pl.when(k == 3)
            def _():
                stat_next(0, 1)

        loop(3, lambda k: serve_far_all(k + 1))

        def take_grand():
            exchanged(*stat(0, 2)).wait_recv()
            total = added(stats.at[0, 2])
            for which in (0, 1):
                grand[which : which + 1, :] = total[which, :, :width] / total[which, 0, width]
            for d in (1, 2):
                exchanged(*ring(d)).wait_recv()

            def late_left(j):
                cs = cs_of(j)
                mean = grand[0:1, cs]
                rows = [
                    packed([rings[d, m, 0, :, cs] - rings[d, m, 0, :, tail] * mean for m in range(4)], True) for d in range(3)
                ]
                put_left(j, pl.ds(depth, AUX), filled(jnp.concatenate(rows, axis=0)))

            loop_by(width // LANE, 4, late_left)
            late_push.start()
            for q in range(3):
                d = axes[q][0]

                def late_right(cs):
                    mean = grand[1:2, cs]
                    rows = packed([rings[d, m, 1, :, cs] / rings[d, m, 1, :, tail] - mean for m in range(4)], False)
                    rows = jnp.concatenate([jnp.where(d == k, rows, 0.0) for k in range(3)], axis=0)
                    right[pl.ds(depth, AUX), cs] = filled(rows).astype(jnp.bfloat16)

                each_tile(q, late_right)

            eight = lax.broadcasted_iota(jnp.int32, (8, LANE), 0)
            weight_rows = jnp.zeros((8, LANE), jnp.float32)
            for w in range(4):
                weight_rows = jnp.where(eight == w, count[w], weight_rows)
            count_rows = jnp.maximum(weight_rows, 1.0)

            def spread(j):
                cs = cs_of(j)
                for which in (0, 1):
                    shift = sums_of[which, :, cs] / count_rows - grand[which : which + 1, cs]
                    part = squares[which, :, cs] + weight_rows * shift * shift
                    stats[1, 0, me[0], which, :, cs] = jnp.sum(part, axis=0, keepdims=True)

            for which in (0, 1):
                stats[1, 0, me[0], which, :, tail] = jnp.zeros((1, LANE), jnp.float32)
            loop(width // LANE, spread)
            exchange(*stat(1, 0))

        mid_out = far_out

        def mid(q, n, way=0):
            cs = columns(q)
            lines = (upper, lower)[way] if n == 0 else pl.ds(0, rows)
            k = way if n == 0 else n + 1
            step = (1, 3)[way] if n == 0 else (1, 3)[n - 1]
            return pair(
                mid_out.at[n, lines, cs], mid_in.at[n, lines, cs], mid_scale.at[n, :, cs], mid_scale_in.at[k, :, cs],
                mid_sems, q, k // 2, device(q, 1, step),
            )

        def merged(k, cs):
            n = 2 * k
            return (
                acc[k, :, cs]
                + decoded(near_in.at[n, :, cs], near_scale_in.at[n, :, cs])
                + decoded(near_in.at[n + 1, :, cs], near_scale_in.at[n + 1, :, cs])
            )

        def take_own(k, groups_of=(0, 1, 2)):
            for q in groups_of:
                arrived(near_both(q, k))
                if k == 1:
                    arrived(mid_both(q, 0))

                def body(cs):
                    p = merged(k, cs)
                    if k == 3:
                        sums[:, cs] = p
                        return
                    if k == 1:
                        more = decoded(mid_in.at[0, upper, cs], mid_scale_in.at[0, :, cs])
                        p = jnp.concatenate([p[: rows // 2] + more, p[rows // 2 :]], axis=0)
                    if k == 2:
                        more = decoded(mid_in.at[0, lower, cs], mid_scale_in.at[1, :, cs])
                        p = jnp.concatenate([p[: rows // 2], p[rows // 2 :] + more], axis=0)
                    encoded(p, mid_out.at[k, :, cs], mid_scale.at[k, :, cs])

                each_tile(q, body)
                if k == 0:
                    start(mid(q, 0, 0))
                    start(mid(q, 0, 1))
                elif k < 3:
                    start(mid(q, k))

        def serve(k):
            serve_near(k)

            @pl.when(k == 1)
            def _():
                take_grand()
                gone(far_all())

            @pl.when(k == 2)
            def _():
                late_push.wait_recv()

            @pl.when(k >= 2)
            def _():
                for q in range(3):
                    multiply_own(q, distance_of(k - 2), acc.at[k - 2])

            for before in range(2):

                @pl.when(k == before + 2)
                def _():
                    take_own(before)

            @pl.when(k == 3)
            def _():
                stat_next(1, 0)
                for q in range(3):
                    multiply_own(q, DISTANCES[2], acc.at[2])

        loop(4, serve)
        take_own(2)
        for q in range(3):
            multiply_own(q, 0)
        stat_next(1, 1)

        part = rows // 4
        half = part // 2
        front, back = pl.ds(0, half), pl.ds(half, half)

        def last(q, n, way):
            cs = columns(q)
            lines = (front, back)[way]
            step = (1, 3)[way] if n == 0 else (1, 3)[n - 1]
            return pair(
                last_out.at[n, lines, cs], last_in.at[n, lines, cs],
                last_scale.at[2 * n + way, :, cs], last_scale_in.at[2 * n + way, :, cs],
                last_sems, q, min(n, 1), device(q, 2, step),
            )

        def put_last(p, n, way, cs):
            encoded(p, last_out.at[n, (front, back)[way], cs], last_scale.at[2 * n + way, :, cs])

        for q in range(3):
            take_own(3, (q,))
            arrived(mid_both(q, 1))

            def body(cs):
                p = (
                    sums[:, cs]
                    + decoded(mid_in.at[1, :, cs], mid_scale_in.at[2, :, cs])
                    + decoded(mid_in.at[2, :, cs], mid_scale_in.at[3, :, cs])
                )
                put_last(p[:half], 0, 0, cs)
                put_last(p[half:part], 0, 1, cs)
                put_last(p[part + half : 2 * part], 1, 1, cs)
                put_last(p[2 * part : 2 * part + half], 2, 0, cs)
                sums[pl.ds(part, 3 * part), cs] = p[part:]

            each_tile(q, body)
            for n, way in ((0, 0), (0, 1), (1, 1), (2, 0)):
                start(last(q, n, way))

        for q in range(3):
            arrived(last_both(q, 0))

            def body(cs):
                ahead = sums[pl.ds(part, half), cs] + decoded(last_in.at[0, front, cs], last_scale_in.at[0, :, cs])
                put_last(ahead, 1, 0, cs)
                behind = sums[pl.ds(2 * part + half, half), cs] + decoded(
                    last_in.at[0, back, cs], last_scale_in.at[1, :, cs]
                )
                put_last(behind, 2, 1, cs)

            each_tile(q, body)
            start(last(q, 1, 0))
            start(last(q, 2, 1))

        exchanged(*stat(1, 2)).wait_recv()
        spread_first[core] = added(stats.at[1, 2])
        spread_push.start()
        spread_push.wait_recv()
        grand_count = added(stats.at[0, 2])[0, 0, width]
        row_block = me[0] * 16 + me[1] * 4 + me[2]
        in_half = lax.rem(row_block, half_blocks)
        lane_block = cs_of(in_half * block // LANE)
        line = spread_first[row_block // half_blocks, 0, :, lane_block] / grand_count
        column[...] = jnp.broadcast_to(line, (LANE, LANE)).T
        rows_var = column[pl.ds(pl.multiple_of(lax.rem(in_half, groups) * block, block), block), :] + 0.1

        for q in range(3):
            arrived(last_both(q, 1))

            def body(cs):
                halves = []
                for way, lines in ((0, front), (1, back)):
                    halves.append(
                        sums[pl.ds(3 * part + way * half, half), cs]
                        + decoded(last_in.at[1, lines, cs], last_scale_in.at[2 + way, :, cs])
                        + decoded(last_in.at[2, lines, cs], last_scale_in.at[4 + way, :, cs])
                    )
                cross = jnp.concatenate(halves, axis=0)
                columns_var = spread_first[core, 1, :, cs] / grand_count + 0.1
                out_ref[pl.ds(0, block), cs] = cross / grand_count * lax.rsqrt(rows_var * columns_var)

            each_tile(q, body)

        out_ref[pl.ds(block, 2), :] = grand[0:2, :]

        for copies in (near_all(), mid_all(), last_all()):
            gone(copies)
        for copy in (main_push, late_push, spread_push):
            copy.wait_send()
        for d in range(3):
            exchanged(*ring(d)).wait_send()
            exchanged(*stat(1, d)).wait_send()
            if d > 0:
                exchanged(*stat(0, d)).wait_send()

    pl.run_scoped(prepare, pltpu.VMEM((tokens, width), jnp.bfloat16))
    pl.run_scoped(reduce, pltpu.VMEM((4, rows, width), jnp.float32))


def local(first_acts, second_acts, window_counts):
    tokens, width = first_acts.shape
    block = width * lax.axis_size("col") // lax.axis_size(TOK)
    blocks = width // block
    rows, depth = 4 * block, tokens + 2 * AUX
    i16, f32, bf16 = jnp.int16, jnp.float32, jnp.bfloat16
    dma = pltpu.SemaphoreType.DMA
    vmem = pltpu.VMEM
    out = pl.pallas_call(
        functools.partial(kernel, widths_of(width)),
        out_shape=jax.ShapeDtypeStruct((block + 8, width), f32),
        in_specs=[
            pl.BlockSpec(memory_space=pltpu.SMEM),
            pl.BlockSpec(memory_space=pl.ANY),
            pl.BlockSpec(memory_space=pl.ANY),
        ],
        out_specs=pl.BlockSpec(memory_space=vmem),
        scratch_shapes=[
            vmem((2 * blocks, block, depth), bf16),
            vmem((depth, width), bf16),
            vmem((4, rows, width), i16), vmem((4, rows, width), i16),
            vmem((8, rows, width), i16), vmem((8, rows, width), i16),
            vmem((3, block, width), i16), vmem((3, block, width), i16),
            vmem((3, rows, width), i16),
            vmem((4, 1, width), f32), vmem((8, 1, width), f32),
            vmem((8, 1, width), f32), vmem((8, 1, width), f32),
            vmem((3, 1, width), f32), vmem((4, 1, width), f32),
            vmem((6, 1, width), f32), vmem((6, 1, width), f32),
            vmem((2, 8, width), f32), vmem((2, 8, width), f32), vmem((tokens // 4, LANE), bf16),
            vmem((3, 4, 2, 1, width + LANE), f32),
            vmem((2, 3, 4, 2, 1, width + LANE), f32),
            vmem((2, 2, 1, width + LANE), f32),
            vmem((8, width), f32),
            vmem((LANE, LANE), f32),
            dma((2, 4)), dma((3,)), dma((3,)),
            dma((3,)), dma((3,)), dma((2, 3)), dma((2, 3)),
            dma((1,)), dma((1, 4)), dma((1,)), dma((1, 4)),
            dma((1,)), dma((3, 4)), dma((1,)), dma((3, 4)),
            dma((1,)), dma((3, 2)), dma((1,)), dma((3, 2)),
            dma((1,)), dma((3, 2)), dma((1,)), dma((3, 2)),
        ],
        compiler_params=pltpu.CompilerParams(
            collective_id=0, has_side_effects=True, vmem_limit_bytes=67_043_328
        ),
        cost_estimate=pl.CostEstimate(
            flops=4 * width * width * depth, bytes_accessed=30_000_000, transcendentals=0
        ),
        name="whole",
    )(window_counts, first_acts, second_acts)

    def cut(out_ref, whitened_ref, means_ref):
        whitened_ref[...] = out_ref[:block]
        means_ref[...] = out_ref[block : block + 2]

    return tuple(
        pl.pallas_call(
            cut,
            out_shape=(jax.ShapeDtypeStruct((block, width), f32), jax.ShapeDtypeStruct((2, width), f32)),
            name="cut",
        )(out)
    )


def solution(mesh):
    torus = Mesh(
        mesh.devices.reshape(4, 4, 4, mesh.shape["col"]), ("tok_0", "tok_1", "tok_2", "col")
    )
    return jax.shard_map(
        local,
        mesh=torus,
        in_specs=(P(TOK, "col"), P(TOK, "col"), P(TOK)),
        out_specs=(P(TOK, "col"), P(None, "col")),
        check_vma=False,
    )
```

```python
import functools

import jax
import jax.numpy as jnp
from jax import lax
from jax.experimental import pallas as pl
from jax.experimental.pallas import tpu as pltpu
from jax.sharding import Mesh
from jax.sharding import PartitionSpec as P

TOK = ("tok_0", "tok_1", "tok_2")
MESH = pl.DeviceIdType.MESH
LANE = 128
AUX = 128
CODES = 32767.0

DISTANCES = (2, 1, 3, 0)


def widths_of(width):
    tiles = width // LANE
    return [(tiles // 3 + (1 if q < tiles % 3 else 0)) * LANE for q in range(3)]


def pick(k, values):
    result = values[-1]
    for n in range(len(values) - 2, -1, -1):
        result = jnp.where(k == n, values[n], result)
    return result


def kernel(
    widths,
    counts_ref, first_hbm, second_hbm, out_ref,
    left, right, far_out, far_in, near_out, near_in, last_out, last_in, mid_in,
    far_scale, far_scale_in, near_scale, near_scale_in, mid_scale, mid_scale_in, last_scale, last_scale_in,
    sums_of, squares, live_slots, rings, stats, spread_first, grand, column,
    load_sem, peer_send, peer_recv, ring_send, ring_recv, stat_send, stat_recv,
    far_s, far_r, far_t, far_u, near_s, near_r, near_t, near_u,
    mid_s, mid_r, mid_t, mid_u, last_s, last_r, last_t, last_u,
):
    me = [lax.axis_index(name) for name in TOK]
    core = lax.axis_index("col")
    width = right.shape[1]
    tokens = first_hbm.shape[0]
    depth = tokens + AUX
    slots = tokens // 4
    half_blocks = left.shape[0] // 2
    block = left.shape[1]
    starts = [sum(widths[:q]) for q in range(3)]
    rows = far_out.shape[1]
    upper, lower = pl.ds(0, rows // 2), pl.ds(rows // 2, rows // 2)

    def at(axis, coordinate):
        return {TOK[d]: jnp.where(axis == d, coordinate, me[d]) for d in range(3)}

    other = {"col": 1 - core}

    tail = pl.ds(width, LANE)

    def cs_of(j):
        return pl.ds(pl.multiple_of(j * LANE, LANE), LANE)

    def loop(n, body):
        def step(j, _):
            body(j)
            return 0

        lax.fori_loop(0, n, step, 0)

    def loop_by(n, unroll, body):
        def step(j):
            for i in range(unroll):
                body(j * unroll + i)

        loop(n // unroll, step)

    def exchange(ref, d, send, recv):
        for step in (1, 2, 3):
            pltpu.make_async_remote_copy(
                ref.at[me[d]], ref.at[me[d]], send, recv,
                device_id={TOK[d]: lax.rem(me[d] + step, 4)}, device_id_type=MESH,
            ).start()

    def exchanged(ref, d, send, recv):
        three = ref.at[pl.ds(0, 3)]
        return pltpu.make_async_remote_copy(
            three, three, send, recv, device_id={TOK[d]: lax.rem(me[d] + 1, 4)}, device_id_type=MESH
        )

    def ring(d):
        return rings.at[d], d, ring_send.at[d], ring_recv.at[d]

    def stat(kind, d):
        return stats.at[kind, d], d, stat_send.at[kind, d], stat_recv.at[kind, d]

    def added(ref):
        return ref[0] + ref[1] + ref[2] + ref[3]

    def stat_next(kind, d):
        now = ring(0) if (kind, d) == (0, 0) else stat(kind, d)
        exchanged(*now).wait_recv()
        stats[kind, d + 1, me[d + 1]] = added(now[0])
        exchange(*stat(kind, d + 1))

    mine = pl.ds(core * half_blocks, half_blocks)
    groups = LANE // block

    def push(lanes, k, half=mine):
        return pltpu.make_async_remote_copy(
            left.at[half, :, lanes], left.at[half, :, lanes], peer_send.at[k], peer_recv.at[k],
            device_id=other, device_id_type=MESH,
        )

    main_push = push(pl.ds(0, depth), 0)
    late_push = push(pl.ds(depth, AUX), 1)
    spread_push = pltpu.make_async_remote_copy(
        spread_first.at[core], spread_first.at[core], peer_send.at[2], peer_recv.at[2],
        device_id=other, device_id_type=MESH,
    )

    count = [counts_ref[w].astype(jnp.float32) for w in range(4)]
    device_count = count[0] + count[1] + count[2] + count[3]
    row16 = lax.broadcasted_iota(jnp.int32, (16, LANE), 0)

    def packed(values, weighted):
        result = jnp.zeros((16, LANE), jnp.float32)
        for w, value in enumerate(values):
            high = value.astype(jnp.bfloat16).astype(jnp.float32)
            low = value - high
            order = (high, high, low, low) if weighted else (high, low, high, low)
            for k in range(4):
                result = jnp.where(row16 == 4 * k + w, order[k], result)
        return result

    def put_left(j, lanes, rows):
        turned = rows.T.astype(jnp.bfloat16)
        for k in range(groups):
            left[core * half_blocks + j * groups + k, :, lanes] = turned[k * block : (k + 1) * block]

    def filled(rows):
        return jnp.concatenate([rows, jnp.zeros((AUX - rows.shape[0], LANE), jnp.float32)], axis=0)

    def prepare(raw):
        loads = []
        for w in range(4):
            lines = pl.ds(w * slots, slots)
            loads.append(pltpu.make_async_copy(first_hbm.at[lines], raw.at[lines], load_sem.at[0, w]))
            loads.append(pltpu.make_async_copy(second_hbm.at[lines], right.at[lines], load_sem.at[1, w]))
        for copy in loads:
            copy.start()
        barrier = pltpu.get_barrier_semaphore()
        for d in range(3):
            for step in (1, 2, 3):
                pl.semaphore_signal(
                    barrier, inc=1, device_id={TOK[d]: lax.rem(me[d] + step, 4)}, device_id_type=MESH
                )
        pl.semaphore_signal(barrier, inc=1, device_id=other, device_id_type=MESH)

        row = lax.broadcasted_iota(jnp.int32, (8, slots), 0)
        slot = lax.broadcasted_iota(jnp.int32, (8, slots), 1)
        squares[...] = jnp.zeros_like(squares)
        sums_of[...] = jnp.zeros_like(sums_of)

        def total_of(w):
            live = jnp.where((row == w) & (slot < counts_ref[w]), 1.0, 0.0).astype(jnp.bfloat16)
            for which, ref in ((0, raw), (1, right)):
                loads[2 * w + which].wait()
                sums_of[which] += jnp.dot(
                    live, ref[pl.ds(w * slots, slots), :], preferred_element_type=jnp.float32
                )

        def center(w):
            live = lax.broadcasted_iota(jnp.int32, (slots, LANE), 0) < counts_ref[w]
            live_slots[...] = jnp.where(live, 1.0, 0.0).astype(jnp.bfloat16)
            lines = pl.ds(w * slots, slots)

            def centered_of(ref, which, cs):
                mean = sums_of[which, w : w + 1, cs] / count[w]
                x = (ref[lines, cs].astype(jnp.float32) - mean).astype(jnp.bfloat16) * live_slots[...]
                wide = x.astype(jnp.float32)
                squares[which, :, cs] += jnp.sum((wide * wide).reshape(slots // 8, 8, LANE), axis=0)
                return x

            def chunk(j):
                cs = cs_of(j)
                turned = centered_of(raw, 0, cs).T
                for k in range(groups):
                    left[core * half_blocks + j * groups + k, :, lines] = turned[k * block : (k + 1) * block]
                right[lines, cs] = centered_of(right, 1, cs)

            pieces = (1, 2, 2, 4)[w]
            chunks, step = width // LANE // pieces, half_blocks // pieces
            for piece in range(pieces):
                loop_by(chunks, 2, lambda j: chunk(piece * chunks + j))
                if w == 0:
                    pl.semaphore_wait(barrier, 10)
                push(lines, 0, pl.ds(core * half_blocks + piece * step, step)).start()

        total_of(0)
        center(0)
        for w in (1, 2):
            total_of(w)
            center(w)
        total_of(3)
        for which in (0, 1):
            device_sum = jnp.sum(sums_of[which], axis=0, keepdims=True)
            for d in range(3):
                rings[d, me[d], which, :, pl.ds(0, width)] = device_sum
                rings[d, me[d], which, :, tail] = jnp.full((1, LANE), device_count, jnp.float32)
        for d in range(3):
            exchange(*ring(d))

        def aux_rows(which, cs, weighted):
            device_mean = jnp.sum(sums_of[which, :, cs], axis=0, keepdims=True) / device_count
            values = []
            for w in range(4):
                value = sums_of[which, w : w + 1, cs] / count[w] - device_mean
                values.append(count[w] * value if weighted else value)
            return filled(packed(values, weighted))

        def aux(j):
            cs = cs_of(j)
            put_left(j, pl.ds(tokens, AUX), aux_rows(0, cs, True))
            right[pl.ds(tokens, AUX), cs] = aux_rows(1, cs, False).astype(jnp.bfloat16)

        loop_by(width // LANE, 4, aux)
        push(pl.ds(tokens, AUX), 0).start()
        center(3)
        main_push.wait_recv()

    def reduce(acc):
        sums = acc.at[3]
        axes = [[lax.rem(core + q + k, 3) for k in range(3)] for q in range(3)]
        here = [[pick(axes[q][k], me) for k in range(3)] for q in range(3)]
        stride = [[pick(axes[q][k], (16, 4, 1)) for k in range(3)] for q in range(3)]

        def columns(q):
            return pl.ds(starts[q], widths[q])

        def moved(q, k, step):
            return lax.rem(here[q][k] + step, 4)

        def device(q, k, step):
            return at(axes[q][k], moved(q, k, step))

        def distance_of(k):
            return pick(k, DISTANCES)

        def multiply(q, first_step, second_step, into=None, lanes=depth):
            into = sums if into is None else into
            base = moved(q, 0, first_step) * stride[q][0] + moved(q, 1, second_step) * stride[q][1]
            deep = pl.ds(0, lanes)
            blocks = [left[base + moved(q, 2, distance) * stride[q][2], :, deep] for distance in DISTANCES]
            into[:, columns(q)] = jnp.dot(
                jnp.concatenate(blocks, axis=0), right[deep, columns(q)], preferred_element_type=jnp.float32
            )

        def multiply_own(q, second_step, into=None):
            multiply(q, 0, second_step, into, depth + AUX)

        def encoded(p, code_ref, scale_ref):
            peak = jnp.maximum(jnp.max(jnp.abs(p), axis=0, keepdims=True), 1e-30)
            code = jnp.round(p * (CODES / peak)).astype(jnp.int32)
            code_ref[...] = code.astype(jnp.int16)
            scale_ref[...] = peak * (1.0 / CODES)

        def encode_sums(q, code_ref, scale_ref):
            for cs in tiles(q):
                encoded(sums[:, cs], code_ref.at[:, cs], scale_ref.at[:, cs])

        def tiles(q):
            return [pl.ds(starts[q] + j, LANE) for j in range(0, widths[q], LANE)]

        def decoded(code_ref, scale_ref):
            return code_ref[...].astype(jnp.int32).astype(jnp.float32) * scale_ref[...]

        def each_tile(q, body):
            def step(j):
                body(pl.ds(pl.multiple_of(starts[q] + j * LANE, LANE), LANE))

            loop(widths[q] // LANE, step)

        def pair(code, code_to, scale, scale_to, sems, q, k, to):
            s, r, t, u = sems
            return (
                pltpu.make_async_remote_copy(
                    code, code_to, s.at[0], r.at[q, k], device_id=to, device_id_type=MESH
                ),
                pltpu.make_async_remote_copy(
                    scale, scale_to, t.at[0], u.at[q, k], device_id=to, device_id_type=MESH
                ),
            )

        far_sems = (far_s, far_r, far_t, far_u)
        near_sems = (near_s, near_r, near_t, near_u)
        mid_sems = (mid_s, mid_r, mid_t, mid_u)
        last_sems = (last_s, last_r, last_t, last_u)

        def far(q, k, way):
            cs = columns(q)
            lines = (upper, lower)[way]
            return pair(
                far_out.at[k, lines, cs], far_in.at[k, lines, cs],
                far_scale.at[k, :, cs], far_scale_in.at[2 * k + way, :, cs],
                far_sems, 0, k, device(q, 0, (1, 3)[way]),
            )

        def near(q, n, step):
            cs = columns(q)
            return pair(
                near_out.at[n, :, cs], near_in.at[n, :, cs], near_scale.at[n, :, cs], near_scale_in.at[n, :, cs],
                near_sems, q, n // 2, device(q, 0, step),
            )

        def both(q, k, code, scale, lines, sems, axis):
            cs = pl.ds(0, width) if q is None else columns(q)
            q = 0 if q is None else q
            code, scale = code.at[lines[0], :, cs], scale.at[lines[1], :, cs]
            return pair(code, code, scale, scale, sems, q, k, device(q, axis, 1))

        def far_both(k):
            return both(None, k, far_in, far_scale_in, (pl.ds(k, 1), pl.ds(2 * k, 2)), far_sems, 0)

        def near_both(q, k):
            return both(q, k, near_in, near_scale_in, (pl.ds(2 * k, 2), pl.ds(2 * k, 2)), near_sems, 0)

        def mid_both(q, k):
            return both(q, k, mid_in, mid_scale_in, ((pl.ds(0, 1), pl.ds(1, 2))[k], pl.ds(2 * k, 2)), mid_sems, 1)

        def last_both(q, k):
            return both(q, k, last_in, last_scale_in, ((pl.ds(0, 1), pl.ds(1, 2))[k], (pl.ds(0, 2), pl.ds(2, 4))[k]), last_sems, 2)

        def far_all():
            return both(None, 0, far_in, far_scale_in, (pl.ds(0, 4), pl.ds(0, 8)), far_sems, 0)

        def near_all():
            return both(None, 0, near_in, near_scale_in, (pl.ds(0, 8), pl.ds(0, 8)), near_sems, 0)

        def mid_all():
            return both(None, 0, mid_in, mid_scale_in, (pl.ds(0, 3), pl.ds(0, 4)), mid_sems, 1)

        def last_all():
            return both(None, 0, last_in, last_scale_in, (pl.ds(0, 3), pl.ds(0, 6)), last_sems, 2)

        def start(copies):
            for copy in copies:
                copy.start()

        def arrived(copies):
            for copy in copies:
                copy.wait_recv()

        def gone(copies):
            for copy in copies:
                copy.wait_send()

        def serve_far(k):
            for q in range(3):
                if q < 2:
                    multiply(q + 1, 2, distance_of(k))
                else:
                    multiply(0, jnp.where(k == 3, 1 + 2 * core, 2), pick(k, DISTANCES[1:] + DISTANCES[:1]))
                encode_sums(q, far_out.at[k], far_scale.at[k])
            for q in range(3):
                start(far(q, k, 0))
                start(far(q, k, 1))

        def serve_near(k):
            for turn in (0, 1):
                way = turn + core - 2 * turn * core
                later = 1 - way
                n = 2 * k + way
                lines = pl.ds(pl.multiple_of(way * (rows // 2), rows // 2), rows // 2)
                if turn == 0:
                    arrived(far_both(k))
                for q in range(3):
                    if q < 2:
                        multiply(q + 1, 1 + 2 * way, distance_of(k))
                    elif turn == 0:
                        multiply(0, 1 + 2 * later, distance_of(k))
                    else:
                        multiply(0, jnp.where(k == 3, 0, 1 + 2 * core), pick(k, DISTANCES[1:] + DISTANCES[3:]))
                    for cs in tiles(q):
                        more = decoded(far_in.at[k, lines, cs], far_scale_in.at[n, :, cs])
                        sums[lines, cs] += more
                        encoded(sums[:, cs], near_out.at[n, :, cs], near_scale.at[n, :, cs])
                for q in range(3):
                    start(near(q, n, 1 + 2 * way))

        multiply(0, 2, DISTANCES[0])
        for q in range(3):
            if q < 2:
                multiply(q + 1, 2, DISTANCES[0])
            else:
                multiply(0, 2, DISTANCES[1])
            encode_sums(q, far_out.at[0], far_scale.at[0])
            start(far(q, 0, 0))
            start(far(q, 0, 1))
        stat_next(0, 0)

        def serve_far_all(k):
            serve_far(k)

            @pl.when(k == 3)
            def _():
                stat_next(0, 1)

        loop(3, lambda k: serve_far_all(k + 1))

        def take_grand():
            exchanged(*stat(0, 2)).wait_recv()
            total = added(stats.at[0, 2])
            for which in (0, 1):
                grand[which : which + 1, :] = total[which, :, :width] / total[which, 0, width]
            for d in (1, 2):
                exchanged(*ring(d)).wait_recv()

            def late_left(j):
                cs = cs_of(j)
                mean = grand[0:1, cs]
                rows = [
                    packed([rings[d, m, 0, :, cs] - rings[d, m, 0, :, tail] * mean for m in range(4)], True) for d in range(3)
                ]
                put_left(j, pl.ds(depth, AUX), filled(jnp.concatenate(rows, axis=0)))

            loop_by(width // LANE, 4, late_left)
            late_push.start()
            for q in range(3):
                d = axes[q][0]

                def late_right(cs):
                    mean = grand[1:2, cs]
                    rows = packed([rings[d, m, 1, :, cs] / rings[d, m, 1, :, tail] - mean for m in range(4)], False)
                    rows = jnp.concatenate([jnp.where(d == k, rows, 0.0) for k in range(3)], axis=0)
                    right[pl.ds(depth, AUX), cs] = filled(rows).astype(jnp.bfloat16)

                each_tile(q, late_right)

            eight = lax.broadcasted_iota(jnp.int32, (8, LANE), 0)
            weight_rows = jnp.zeros((8, LANE), jnp.float32)
            for w in range(4):
                weight_rows = jnp.where(eight == w, count[w], weight_rows)
            count_rows = jnp.maximum(weight_rows, 1.0)

            def spread(j):
                cs = cs_of(j)
                for which in (0, 1):
                    shift = sums_of[which, :, cs] / count_rows - grand[which : which + 1, cs]
                    part = squares[which, :, cs] + weight_rows * shift * shift
                    stats[1, 0, me[0], which, :, cs] = jnp.sum(part, axis=0, keepdims=True)

            for which in (0, 1):
                stats[1, 0, me[0], which, :, tail] = jnp.zeros((1, LANE), jnp.float32)
            loop(width // LANE, spread)
            exchange(*stat(1, 0))

        mid_out = far_out

        def mid(q, n, way=0):
            cs = columns(q)
            lines = (upper, lower)[way] if n == 0 else pl.ds(0, rows)
            k = way if n == 0 else n + 1
            step = (1, 3)[way] if n == 0 else (1, 3)[n - 1]
            return pair(
                mid_out.at[n, lines, cs], mid_in.at[n, lines, cs], mid_scale.at[n, :, cs], mid_scale_in.at[k, :, cs],
                mid_sems, q, k // 2, device(q, 1, step),
            )

        def merged(k, cs):
            n = 2 * k
            return (
                acc[k, :, cs]
                + decoded(near_in.at[n, :, cs], near_scale_in.at[n, :, cs])
                + decoded(near_in.at[n + 1, :, cs], near_scale_in.at[n + 1, :, cs])
            )

        def take_own(k, groups_of=(0, 1, 2)):
            for q in groups_of:
                arrived(near_both(q, k))
                if k == 1:
                    arrived(mid_both(q, 0))

                def body(cs):
                    p = merged(k, cs)
                    if k == 3:
                        sums[:, cs] = p
                        return
                    if k == 1:
                        more = decoded(mid_in.at[0, upper, cs], mid_scale_in.at[0, :, cs])
                        p = jnp.concatenate([p[: rows // 2] + more, p[rows // 2 :]], axis=0)
                    if k == 2:
                        more = decoded(mid_in.at[0, lower, cs], mid_scale_in.at[1, :, cs])
                        p = jnp.concatenate([p[: rows // 2], p[rows // 2 :] + more], axis=0)
                    encoded(p, mid_out.at[k, :, cs], mid_scale.at[k, :, cs])

                each_tile(q, body)
                if k == 0:
                    start(mid(q, 0, 0))
                    start(mid(q, 0, 1))
                elif k < 3:
                    start(mid(q, k))

        def serve(k):
            serve_near(k)

            @pl.when(k == 1)
            def _():
                take_grand()
                gone(far_all())

            @pl.when(k == 2)
            def _():
                late_push.wait_recv()

            @pl.when(k >= 2)
            def _():
                for q in range(3):
                    multiply_own(q, distance_of(k - 2), acc.at[k - 2])

            for before in range(2):

                @pl.when(k == before + 2)
                def _():
                    take_own(before)

            @pl.when(k == 3)
            def _():
                stat_next(1, 0)
                for q in range(3):
                    multiply_own(q, DISTANCES[2], acc.at[2])

        loop(4, serve)
        take_own(2)
        for q in range(3):
            multiply_own(q, 0)
        stat_next(1, 1)

        part = rows // 4
        half = part // 2
        front, back = pl.ds(0, half), pl.ds(half, half)

        def last(q, n, way):
            cs = columns(q)
            lines = (front, back)[way]
            step = (1, 3)[way] if n == 0 else (1, 3)[n - 1]
            return pair(
                last_out.at[n, lines, cs], last_in.at[n, lines, cs],
                last_scale.at[2 * n + way, :, cs], last_scale_in.at[2 * n + way, :, cs],
                last_sems, q, min(n, 1), device(q, 2, step),
            )

        def put_last(p, n, way, cs):
            encoded(p, last_out.at[n, (front, back)[way], cs], last_scale.at[2 * n + way, :, cs])

        for q in range(3):
            take_own(3, (q,))
            arrived(mid_both(q, 1))

            def body(cs):
                p = (
                    sums[:, cs]
                    + decoded(mid_in.at[1, :, cs], mid_scale_in.at[2, :, cs])
                    + decoded(mid_in.at[2, :, cs], mid_scale_in.at[3, :, cs])
                )
                put_last(p[:half], 0, 0, cs)
                put_last(p[half:part], 0, 1, cs)
                put_last(p[part + half : 2 * part], 1, 1, cs)
                put_last(p[2 * part : 2 * part + half], 2, 0, cs)
                sums[pl.ds(part, 3 * part), cs] = p[part:]

            each_tile(q, body)
            for n, way in ((0, 0), (0, 1), (1, 1), (2, 0)):
                start(last(q, n, way))

        for q in range(3):
            arrived(last_both(q, 0))

            def body(cs):
                ahead = sums[pl.ds(part, half), cs] + decoded(last_in.at[0, front, cs], last_scale_in.at[0, :, cs])
                put_last(ahead, 1, 0, cs)
                behind = sums[pl.ds(2 * part + half, half), cs] + decoded(
                    last_in.at[0, back, cs], last_scale_in.at[1, :, cs]
                )
                put_last(behind, 2, 1, cs)

            each_tile(q, body)
            start(last(q, 1, 0))
            start(last(q, 2, 1))

        exchanged(*stat(1, 2)).wait_recv()
        spread_first[core] = added(stats.at[1, 2])
        spread_push.start()
        spread_push.wait_recv()
        grand_count = added(stats.at[0, 2])[0, 0, width]
        row_block = me[0] * 16 + me[1] * 4 + me[2]
        in_half = lax.rem(row_block, half_blocks)
        lane_block = cs_of(in_half * block // LANE)
        line = spread_first[row_block // half_blocks, 0, :, lane_block] / grand_count
        column[...] = jnp.broadcast_to(line, (LANE, LANE)).T
        rows_var = column[pl.ds(pl.multiple_of(lax.rem(in_half, groups) * block, block), block), :] + 0.1

        for q in range(3):
            arrived(last_both(q, 1))

            def body(cs):
                halves = []
                for way, lines in ((0, front), (1, back)):
                    halves.append(
                        sums[pl.ds(3 * part + way * half, half), cs]
                        + decoded(last_in.at[1, lines, cs], last_scale_in.at[2 + way, :, cs])
                        + decoded(last_in.at[2, lines, cs], last_scale_in.at[4 + way, :, cs])
                    )
                cross = jnp.concatenate(halves, axis=0)
                columns_var = spread_first[core, 1, :, cs] / grand_count + 0.1
                out_ref[pl.ds(0, block), cs] = cross / grand_count * lax.rsqrt(rows_var * columns_var)

            each_tile(q, body)

        out_ref[pl.ds(block, 2), :] = grand[0:2, :]

        for copies in (near_all(), mid_all(), last_all()):
            gone(copies)
        for copy in (main_push, late_push, spread_push):
            copy.wait_send()
        for d in range(3):
            exchanged(*ring(d)).wait_send()
            exchanged(*stat(1, d)).wait_send()
            if d > 0:
                exchanged(*stat(0, d)).wait_send()

    pl.run_scoped(prepare, pltpu.VMEM((tokens, width), jnp.bfloat16))
    pl.run_scoped(reduce, pltpu.VMEM((4, rows, width), jnp.float32))


def local(first_acts, second_acts, window_counts):
    tokens, width = first_acts.shape
    block = width * lax.axis_size("col") // lax.axis_size(TOK)
    blocks = width // block
    rows, depth = 4 * block, tokens + 2 * AUX
    i16, f32, bf16 = jnp.int16, jnp.float32, jnp.bfloat16
    dma = pltpu.SemaphoreType.DMA
    vmem = pltpu.VMEM
    out = pl.pallas_call(
        functools.partial(kernel, widths_of(width)),
        out_shape=jax.ShapeDtypeStruct((block + 8, width), f32),
        in_specs=[
            pl.BlockSpec(memory_space=pltpu.SMEM),
            pl.BlockSpec(memory_space=pl.ANY),
            pl.BlockSpec(memory_space=pl.ANY),
        ],
        out_specs=pl.BlockSpec(memory_space=vmem),
        scratch_shapes=[
            vmem((2 * blocks, block, depth), bf16),
            vmem((depth, width), bf16),
            vmem((4, rows, width), i16), vmem((4, rows, width), i16),
            vmem((8, rows, width), i16), vmem((8, rows, width), i16),
            vmem((3, block, width), i16), vmem((3, block, width), i16),
            vmem((3, rows, width), i16),
            vmem((4, 1, width), f32), vmem((8, 1, width), f32),
            vmem((8, 1, width), f32), vmem((8, 1, width), f32),
            vmem((3, 1, width), f32), vmem((4, 1, width), f32),
            vmem((6, 1, width), f32), vmem((6, 1, width), f32),
            vmem((2, 8, width), f32), vmem((2, 8, width), f32), vmem((tokens // 4, LANE), bf16),
            vmem((3, 4, 2, 1, width + LANE), f32),
            vmem((2, 3, 4, 2, 1, width + LANE), f32),
            vmem((2, 2, 1, width + LANE), f32),
            vmem((8, width), f32),
            vmem((LANE, LANE), f32),
            dma((2, 4)), dma((3,)), dma((3,)),
            dma((3,)), dma((3,)), dma((2, 3)), dma((2, 3)),
            dma((1,)), dma((1, 4)), dma((1,)), dma((1, 4)),
            dma((1,)), dma((3, 4)), dma((1,)), dma((3, 4)),
            dma((1,)), dma((3, 2)), dma((1,)), dma((3, 2)),
            dma((1,)), dma((3, 2)), dma((1,)), dma((3, 2)),
        ],
        compiler_params=pltpu.CompilerParams(
            collective_id=0, has_side_effects=True, vmem_limit_bytes=67_043_328
        ),
        cost_estimate=pl.CostEstimate(
            flops=4 * width * width * depth, bytes_accessed=30_000_000, transcendentals=0
        ),
        name="whole",
    )(window_counts, first_acts, second_acts)

    def cut(out_ref, whitened_ref, means_ref):
        whitened_ref[...] = out_ref[:block]
        means_ref[...] = out_ref[block : block + 2]

    return tuple(
        pl.pallas_call(
            cut,
            out_shape=(jax.ShapeDtypeStruct((block, width), f32), jax.ShapeDtypeStruct((2, width), f32)),
            name="cut",
        )(out)
    )


def solution(mesh):
    torus = Mesh(
        mesh.devices.reshape(4, 4, 4, mesh.shape["col"]), ("tok_0", "tok_1", "tok_2", "col")
    )
    return jax.shard_map(
        local,
        mesh=torus,
        in_specs=(P(TOK, "col"), P(TOK, "col"), P(TOK)),
        out_specs=(P(TOK, "col"), P(None, "col")),
        check_vma=False,
    )
```
